32 devices in a mesh: group: 8 (over z, core), member: 4 (over y, x).
Axes of the slice: x: 2, y: 2, z: 4, core: 2. Of those that a mesh axis runs over, the one named last changes fastest.
Arguments:
- source: float32 [256, 128, 128], P('group', 'member'), may hold values from -5 to 8
- potential: float32 [256, 128, 128], P('group', 'member'), may hold values from -3 to 3
- refined: int32 [8, 4, 4], P('group', 'member'), may hold values 0 or 1
Outputs:
- smoothed: float32 [256, 128, 128], P('group', 'member')
- residual: float32 [256, 128, 128], P('group', 'member')
The draws below stay inside these ranges and needn't reach their ends.
Inputs may be any that keep to these rules, and one draw needn't show every extreme that they name: 1 marks a refined box, 0 one that is not smoothed on the fine level.
All inputs are finite; a program needn't handle non-finite values. No bound on the sum of `refined` on one device may be relied on, other than what follows from the above.
Results may differ from the reference program's by a relative error of at most 0.000035.
Values sent between devices are 32-bit elements; how exact they have to be, the bound alone decides.
A program may use at most 128 MiB of HBM per device.

```python
import jax
import jax.numpy as jnp
from jax import lax

BOX = 32
NZB = 4
PRE = 2
POST = 2
COARSE = 2
NX = 256
NY = 128
NZ = 128
N_GROUP = 8
N_MEMBER = 4


def draw_source(key, part):
    key_noise = jax.random.fold_in(key, 11)
    shape = (NX, NY, NZ)
    along_x = lax.broadcasted_iota(jnp.float32, shape, 0) / (NX - 1.0)
    along_y = lax.broadcasted_iota(jnp.float32, shape, 1) / (NY - 1.0)
    noise = jnp.clip(jax.random.normal(key_noise, shape, jnp.float32), -4.0, 4.0)
    offset = 1.0 + along_x + along_y
    return (noise + offset).astype(jnp.float32)


def set_ends(entries, key, smallest, high):
    shape = entries.shape
    index_at = [jax.random.randint(jax.random.fold_in(key, axis), (), 0, shape[axis]) for axis in range(len(shape))]
    entries = entries.at[tuple(index_at)].set(smallest)
    longest = shape.index(max(shape))
    index_at[longest] = (index_at[longest] + 1) % shape[longest]
    return entries.at[tuple(index_at)].set(high)


def levels(key, dims, pieces, low, high):
    def one(axis_at, parts):
        draws = jax.random.uniform(jax.random.fold_in(jax.random.fold_in(key, 6), axis_at), (parts,), jnp.float32, low / len(pieces), high / len(pieces))
        return jnp.repeat(jnp.exp(draws), dims[axis_at] // parts).reshape((-1,) + (1,) * (len(dims) - axis_at - 1))

    gain = one(*pieces[0])
    for cut in pieces[1:]:
        gain = gain * one(*cut)
    return gain


def normal_values(stream_key, dims, deviation, most, shards=(), held_as=jnp.bfloat16):
    array = deviation * jax.random.normal(stream_key, dims, jnp.float32)
    if shards:
        array = array * levels(stream_key, dims, shards, -0.22, 0.18)
    return jnp.clip(array, -most, most).astype(held_as)


def setup_inputs(seed: int = 0) -> dict:
    keys = jax.random.split(jax.random.key(seed), 4)
    source = draw_source(jax.random.fold_in(keys[3], 71), 0)
    potential = normal_values(keys[1], (NX, NY, NZ), 0.5, 3.0, ((0, 8), (1, 4)), jnp.float32)
    refined = set_ends((jax.random.randint(keys[2], (N_GROUP, N_MEMBER, NZB), 0, 4) < 3).astype(jnp.int32), jax.random.fold_in(keys[2], 1), 0, 1)
    return {"source": source, "potential": potential, "refined": refined}


def neighbour_sum(grid_field):
    padded = jnp.pad(grid_field, 1)
    total = padded[2:, 1:-1, 1:-1] + padded[:-2, 1:-1, 1:-1]
    total = total + padded[1:-1, 2:, 1:-1] + padded[1:-1, :-2, 1:-1]
    return total + padded[1:-1, 1:-1, 2:] + padded[1:-1, 1:-1, :-2]


def expand(values_in, factor):
    size_a, size_b, size_c = values_in.shape
    wide = jnp.broadcast_to(values_in[:, None, :, None, :, None], (size_a, factor, size_b, factor, size_c, factor))
    return wide.reshape(size_a * factor, size_b * factor, size_c * factor)


def parity_of(shape):
    along_x = lax.broadcasted_iota(jnp.int32, shape, 0)
    along_y = lax.broadcasted_iota(jnp.int32, shape, 1)
    along_z = lax.broadcasted_iota(jnp.int32, shape, 2)
    return (along_x + along_y + along_z) % 2


def red_black(grid_field, right_side, active, parity):
    for colour in (0, 1):
        update = (right_side + neighbour_sum(grid_field)) / 6.0
        grid_field = jnp.where((parity == colour) & active, update, grid_field)
    return grid_field


def reference(source, potential, refined):
    density_mean = jnp.sum(source) / (NX * NY * NZ)
    contrast = source - density_mean
    active = expand(refined == 1, BOX)
    parity = parity_of(source.shape)
    phi = potential
    for _ in range(PRE):
        phi = red_black(phi, contrast, active, parity)
    fine_residual = contrast - (6.0 * phi - neighbour_sum(phi))
    size_a, size_b, size_c = fine_residual.shape
    coarse_source = fine_residual.reshape(size_a // 2, 2, size_b // 2, 2, size_c // 2, 2).sum(axis=(1, 3, 5)) * 0.5
    coarse_parity = parity_of(coarse_source.shape)
    correction = jnp.zeros(coarse_source.shape, jnp.float32)
    for _ in range(COARSE):
        correction = red_black(correction, coarse_source, True, coarse_parity)
    phi = phi + expand(correction, 2)
    for _ in range(POST):
        phi = red_black(phi, contrast, active, parity)
    residual = contrast - (6.0 * phi - neighbour_sum(phi))
    return phi, residual
```

```python
import contextlib
import functools

import jax
import jax.numpy as jnp
from jax import lax
from jax.experimental import pallas as pl
from jax.experimental.pallas import tpu as pltpu
from jax.sharding import PartitionSpec as P

SWEEPS = 2
COARSE = 2
REACH = 2 * SWEEPS
HALO = (REACH + 2) // 2
COARSE_REACH = 2 * COARSE - 1 + (REACH + 2) // 2
COARSE_HALO = COARSE_REACH // 2
ROW0 = 8 + REACH
CROW0 = 16
CPLANE0 = COARSE_HALO + 1
SIDES = ((0, -1), (0, 1), (-1, 0), (1, 0), (-1, -1), (-1, 1), (1, -1), (1, 1))
MESH = pl.DeviceIdType.MESH
SIXTH = 1.0 / 6.0


def phase(name):
    return contextlib.nullcontext()


def span(side, begin, end, first, count):
    if side == 0:
        return pl.ds(first, count), pl.ds(first, count)
    if side > 0:
        return pl.ds(first + count - end, end - begin), pl.ds(first - end, end - begin)
    return pl.ds(first + begin, end - begin), pl.ds(first + count + begin, end - begin)


def kernel(
    dims, sizes,
    refined_ref, source_ref, potential_ref,
    smoothed_ref, residual_ref,
    raw, field, own_rhs, red, mid, landed, defect, pair_rows, mixed, rhs0, rhs1, corr0, corr1, wide,
    flags, active, inside, member_sums, group_sums, dummy,
    local_sem, send_sem, recv_sem, sum_sem,
):
    groups, members = dims
    cx, cy, cz = sizes
    px, hx, hy = cx // 2, cx // 4, cy // 2
    group_at = lax.axis_index("group")
    member_at = lax.axis_index("member")
    f32 = jnp.float32
    black, mix, black_rhs = field.at[0], field.at[1], field.at[2]
    own_rows = pl.ds(ROW0, cy)
    window = cy + 2 * REACH
    cwindow = hy + 16

    load_source = pltpu.make_async_copy(source_ref, raw.at[0], local_sem.at[0])
    load_potential = pltpu.make_async_copy(potential_ref, raw.at[1], local_sem.at[1])
    load_source.start()
    load_potential.start()

    def there(dx, dy):
        ok = None
        for side, at, count in ((dx, group_at, groups), (dy, member_at, members)):
            if side == 0:
                continue
            here = at > 0 if side < 0 else at < count - 1
            ok = here if ok is None else ok & here
        return ok

    def device(dx, dy):
        return (group_at + dx, member_at + dy)

    blank = jnp.zeros((8, cz), f32)
    blank_rows = jnp.zeros((cy, cz), f32)
    for kind in range(2):
        for p in range(px + 2 * HALO):
            field[kind, p, pl.ds(ROW0 - 8, 8), :] = blank
            field[kind, p, pl.ds(ROW0 + cy, 8), :] = blank
        for p in range(HALO):
            field[kind, p, own_rows, :] = blank_rows
            field[kind, HALO + px + p, own_rows, :] = blank_rows
    for x in range(3):
        for y in range(3):
            flags[x, y] = blank

    barrier = pltpu.get_barrier_semaphore()
    for o in range(1, members):
        pl.semaphore_signal(barrier, inc=1, device_id=(group_at, lax.rem(member_at + o, members)), device_id_type=MESH)
    for o in range(1, groups):
        pl.semaphore_signal(barrier, inc=1, device_id=(lax.rem(group_at + o, groups), member_at), device_id_type=MESH)
    expected = jnp.int32(groups - 1 + members - 1)
    for dx, dy in SIDES:
        if dx and dy:
            @pl.when(there(dx, dy))
            def _():
                pl.semaphore_signal(barrier, inc=1, device_id=device(dx, dy), device_id_type=MESH)
            expected = expected + there(dx, dy).astype(jnp.int32)

    for p in range(px + 2 * HALO):
        landed[p, pl.ds(ROW0 - 8, 8), :] = blank
        landed[p, pl.ds(ROW0 + cy, 8), :] = blank
    for p in range(HALO):
        landed[p, own_rows, :] = blank_rows
        landed[HALO + px + p, own_rows, :] = blank_rows
    blank_coarse = jnp.zeros((cwindow, cz), f32)
    for a in range(hx + 2 * CPLANE0):
        mixed[a, pl.ds(CROW0 - 8, cwindow), :] = blank_coarse
    for a in (0, hx + 2 * CPLANE0 - 1):
        corr0[a, pl.ds(CROW0 - 8, cwindow), :] = blank_coarse

    lane8 = lax.broadcasted_iota(jnp.int32, (8, cz), 1)
    boxes = refined_ref.shape[2]
    box = cz // boxes
    marks = jnp.zeros((8, cz), jnp.int32)
    for b in range(boxes):
        marks = jnp.where(lane8 // box == b, jnp.full((8, cz), refined_ref[0, 0, b], jnp.int32), marks)
    flags[1, 1] = (marks == 1).astype(f32)

    crow = lax.broadcasted_iota(jnp.int32, (cwindow, cz), 0) - 8
    clow = jnp.where(member_at > 0, -8, 0)
    chigh = jnp.where(member_at < members - 1, hy + 8, hy)
    within = jnp.where((crow >= clow) & (crow < chigh), SIXTH, 0.0)
    for region in range(3):
        alive = 1.0 if region == 1 else there(region - 1, 0).astype(f32)
        inside[region] = within * alive

    def checker(rows, start=0, lanes_per=1):
        r = lax.broadcasted_iota(jnp.int32, (rows, cz), 0) + start
        return ((r + lax.broadcasted_iota(jnp.int32, (rows, cz), 1) // lanes_per) & 1) == 0

    lane_even = lax.broadcasted_iota(jnp.int32, (8, cz), 1) % 2 == 0

    def wide_mask(rows):
        return lax.broadcasted_iota(jnp.int32, (rows, cz), 1) % 2 == 0

    with phase("load"):
        load_source.wait()
        load_potential.wait()

    with phase("pack"):
        here = checker(cy)
        smooth_own = jnp.broadcast_to(flags[1, 1, 0:1, :], (cy, cz)) > 0.5
        acc = [jnp.zeros((8, cz), f32)] * 4
        for a in range(px):
            s0, s1 = raw[0, 2 * a], raw[0, 2 * a + 1]
            v0, v1 = raw[1, 2 * a], raw[1, 2 * a + 1]
            both = s0 + s1
            acc = [acc[t] + sum(both[8 * u:8 * u + 8] for u in range(t, cy // 8, 4)) for t in range(4)]
            red_rhs = jnp.where(here, s0, s1)
            own_rhs[a] = red_rhs
            mix[HALO + a, own_rows, :] = jnp.where(smooth_own, red_rhs, jnp.where(here, v0, v1))
            black[HALO + a, own_rows, :] = jnp.where(here, v1, v0)
            black_rhs[HALO + a, own_rows, :] = jnp.where(here, s1, s0)
        member_sums[0] = (acc[0] + acc[1]) + (acc[2] + acc[3])

    with phase("barrier"):
        pl.semaphore_wait(barrier, expected)

    def sum_copies(slots, n, count, target):
        return [
            pltpu.make_async_remote_copy(
                src_ref=slots.at[0], dst_ref=slots.at[o], send_sem=sum_sem.at[n], recv_sem=sum_sem.at[n + 1],
                device_id=target(o), device_id_type=MESH,
            )
            for o in range(1, count)
        ]

    def sum_total(slots, n, count):
        others = slots.at[pl.ds(1, count - 1)]
        return pltpu.make_async_remote_copy(
            src_ref=others, dst_ref=others, send_sem=sum_sem.at[n], recv_sem=sum_sem.at[n + 1],
            device_id=(group_at, member_at), device_id_type=MESH,
        )

    def next_member(o):
        return (group_at, lax.rem(member_at + o, members))

    def next_group(o):
        return (lax.rem(group_at + o, groups), member_at)

    def face_copies(kind, n, pairs):
        dx, dy = SIDES[n]
        return [
            pltpu.make_async_remote_copy(
                src_ref=src, dst_ref=dst, send_sem=send_sem.at[kind, n], recv_sem=recv_sem.at[kind, n],
                device_id=device(dx, dy), device_id_type=MESH,
            )
            for src, dst in pairs
        ]

    def first_round(n):
        dx, dy = SIDES[n]
        pairs = [(flags.at[1, 1], flags.at[1 - dx, 1 - dy])]
        rows = 8
        if dx and dy:
            pieces = ((0, 3, 0, 1, 4), (0, 2, 1, 2, 2))
        elif dx:
            pieces = ((0, 1, 0, HALO, cy), (1, 2, 0, HALO - 1, cy))
        else:
            pieces = ((0, 1, 0, px, REACH + 1), (1, 1, 0, px, REACH), (2, 1, 0, px, REACH - 1))
        for kind, kinds, begin, end, deep in pieces:
            sx, tx = span(dx, begin, end, HALO, px)
            sy, ty = span(dy, 0, deep, ROW0, cy)
            pairs.append((field.at[pl.ds(kind, kinds), sx, sy], field.at[pl.ds(kind, kinds), tx, ty]))
            rows += kinds * (end - begin) * deep
        return 0, pairs, rows

    def second_coarse(n):
        dx, dy = SIDES[n]
        if dx and dy:
            pieces = ((0, 1, 5), (1, 3, 3))
        elif dx:
            pieces = ((0, COARSE_HALO, hy),)
        else:
            pieces = ((0, hx, COARSE_REACH),)
        pairs, rows = [], 0
        for begin, end, deep in pieces:
            sx, tx = span(dx, begin, end, CPLANE0, hx)
            sy, ty = span(dy, 0, deep, CROW0, hy)
            pairs.append((mixed.at[sx, sy], mixed.at[tx, ty]))
            rows += (end - begin) * deep
        return 1, pairs, rows

    def second_fine(n):
        dx, dy = SIDES[n]
        if dx and dy:
            pieces = ((0, 1, 0, 4), (1, 2, 0, 2))
        elif dx:
            pieces = ((0, HALO, 0, cy),)
        else:
            pieces = ((0, px, 1, REACH + 1),)
        pairs, rows = [], 0
        for begin, end, skip, deep in pieces:
            sx, tx = span(dx, begin, end, HALO, px)
            sy, ty = span(dy, skip, deep, ROW0, cy)
            pairs.append((mid.at[sx, sy], landed.at[tx, ty]))
            rows += (end - begin) * (deep - skip)
        return 2, pairs, rows

    def start(round_of):
        for n, (dx, dy) in enumerate(SIDES):
            @pl.when(there(dx, dy))
            def _():
                kind, pairs, rows = round_of(n)
                for c in face_copies(kind, n, pairs):
                    c.start()

    def all_of(round_of, n):
        kind, pairs, rows = round_of(n)
        return face_copies(kind, n, [(dummy.at[pl.ds(0, rows)], dummy.at[pl.ds(0, rows)])])[0]

    def arrive(round_of):
        for n, (dx, dy) in enumerate(SIDES):
            @pl.when(there(-dx, -dy))
            def _():
                all_of(round_of, n).wait_recv()

    def sent(round_of):
        for n, (dx, dy) in enumerate(SIDES):
            @pl.when(there(dx, dy))
            def _():
                all_of(round_of, n).wait_send()

    with phase("start1"):
        for c in sum_copies(member_sums, 0, members, next_member):
            c.start()
        start(first_round)

    with phase("w_msum"):
        sum_total(member_sums, 0, members).wait_recv()
    part = member_sums[0]
    for o in range(1, members):
        part = part + member_sums[o]
    group_sums[0] = part
    for c in sum_copies(group_sums, 2, groups, next_group):
        c.start()
    with phase("w_gsum"):
        sum_total(group_sums, 2, groups).wait_recv()
    with phase("mean"):
        total = group_sums[0]
        for o in range(1, groups):
            total = total + group_sums[o]
        mean = jnp.sum(total) / (cx * cy * cz * groups * members)
    with phase("w_halo1"):
        arrive(first_round)

    with phase("masks"):
        edge = lax.broadcasted_iota(jnp.int32, (8, cz), 0) < REACH
        for x in range(3):
            low, own, high = flags[x, 0], flags[x, 1], flags[x, 2]
            low, own, high = (jnp.broadcast_to(v[0:1], (8, cz)) for v in (low, own, high))
            active[x, pl.ds(0, 8), :] = jnp.where(edge, low, own)
            for t in range(1, window // 8 - 1):
                active[x, pl.ds(8 * t, 8), :] = own
            active[x, pl.ds(window - 8, 8), :] = jnp.where(edge, own, high)

    def lanes(value, step):
        lane = lax.broadcasted_iota(jnp.int32, value.shape, 1)
        low = jnp.where(lane < step, 0.0, pltpu.roll(value, step, 1))
        high = jnp.where(lane >= cz - step, 0.0, pltpu.roll(value, cz - step, 1))
        return low + high

    def neighbours(other, planes, row, rows, colour, mask, step):
        centres = {}
        out = []
        for p in planes:
            for q in (p - 1, p, p + 1):
                if q not in centres:
                    centres[q] = other[q, pl.ds(row, rows), :]
            near, far = (centres[p - 1], centres[p + 1]) if colour == 0 else (centres[p + 1], centres[p - 1])
            total = centres[p] + jnp.where(mask, near, far)
            total = total + (other[p, pl.ds(row - 1, rows), :] + other[p, pl.ds(row + 1, rows), :])
            out.append(total + lanes(centres[p], step))
        return out

    fine_mask = checker(window)

    def half_sweep(t, right, old, other, out, also=None):
        colour = t % 2
        wide_by = (REACH - t + 1) // 2
        rows = pl.ds(ROW0 - REACH, window)
        for region, low, high in ((0, HALO - wide_by, HALO), (1, HALO, HALO + px), (2, HALO + px, HALO + px + wide_by)):
            keep = active[region] > 0.5
            for first in range(low, high, 4):
                planes = range(first, min(first + 4, high))
                sums = neighbours(other, planes, ROW0 - REACH, window, colour, fine_mask, 1)
                for p, nbr in zip(planes, sums):
                    total = right[p, rows, :] - mean + nbr
                    before = old[p, rows, :]
                    out[p, rows, :] = jnp.where(keep, total * SIXTH, before)
                    if also is not None and region == 1:
                        also[p - HALO] = jnp.where(keep, 0.0, total - 6.0 * before)

    with phase("pre"):
        half_sweep(0, mix, mix, black, red)
        half_sweep(1, black_rhs, black, red, mid)
        half_sweep(2, mix, mix, mid, red)
        half_sweep(3, black_rhs, black, red, mid, defect)

    own_mask = checker(cy)

    def red_defects(other, planes):
        sums = neighbours(other, [HALO + a for a in planes], ROW0, cy, 0, own_mask, 1)
        for a, nbr in zip(planes, sums):
            centre = red[HALO + a, own_rows, :]
            yield a, centre, own_rhs[a] - mean + nbr - 6.0 * centre

    with phase("restrict"):
        even = wide_mask(cy)
        mixing = checker(hy, 0, 2) ^ jnp.logical_not(wide_mask(hy))
        for first in range(0, px, 4):
            for a, centre, res in red_defects(mid, range(first, first + 4)):
                both = res + defect[a, pl.ds(REACH, cy), :]
                pair_rows[a] = both + jnp.where(even, pltpu.roll(both, cz - 1, 1), pltpu.roll(both, 1, 1))
        for a in range(hx):
            first, second = (
                0.5 * (pair_rows[2 * a + k, pl.ds(0, hy, stride=2), :] + pair_rows[2 * a + k, pl.ds(1, hy, stride=2), :])
                for k in range(2)
            )
            mixed[CPLANE0 + a, pl.ds(CROW0, hy), :] = jnp.where(mixing, first, second)

    with phase("start2"):
        start(second_coarse)
        start(second_fine)
    with phase("w_coarse"):
        arrive(second_coarse)

    with phase("coarse"):
        coarse_rows = pl.ds(CROW0 - 8, cwindow)
        coarse_even = wide_mask(cwindow)
        coarse_mask = checker(cwindow, 0, 2)

        def regions(wide_by):
            first, last = CPLANE0, CPLANE0 + hx
            return (0, first - wide_by, first), (1, first, last), (2, last, last + wide_by)

        for region, low, high in regions(COARSE_HALO):
            weight = inside[region]
            for a in range(low, high):
                both = mixed[a, coarse_rows, :]
                s0 = jnp.where(coarse_even, both, pltpu.roll(both, 1, 1))
                rhs0[a, coarse_rows, :] = s0
                rhs1[a, coarse_rows, :] = jnp.where(coarse_even, pltpu.roll(both, cz - 1, 1), both)
                corr0[a, coarse_rows, :] = s0 * weight
        for t in range(1, 2 * COARSE):
            right, other, out = (rhs1, corr0, corr1) if t % 2 else (rhs0, corr1, corr0)
            for region, low, high in regions((COARSE_REACH - t + 1) // 2):
                weight = inside[region]
                for first in range(low, high, 4):
                    planes = range(first, min(first + 4, high))
                    sums = neighbours(other, planes, CROW0 - 8, cwindow, t % 2, coarse_mask, 2)
                    for a, nbr in zip(planes, sums):
                        out[a, coarse_rows, :] = (right[a, coarse_rows, :] + nbr) * weight

    with phase("w_fine2"):
        arrive(second_fine)
        sent(first_round)

    with phase("prolong"):
        half_rows = hy + 8
        rows = pl.ds(CROW0 - 4, half_rows)
        pick = checker(half_rows, 0, 2)
        low_rows, high_rows = pl.ds(ROW0 - 8, 8), pl.ds(ROW0 + cy, 8)
        sub = lax.broadcasted_iota(jnp.int32, (8, cz), 0)
        for p in range(px + 2 * HALO):
            a, k = CPLANE0 + (p - HALO) // 2, (p - HALO) % 2
            c0, c1 = corr0[a, rows, :], corr1[a, rows, :]
            plane = jnp.where(pick, c1, c0) if k else jnp.where(pick, c0, c1)
            wide[p, pl.ds(0, half_rows, stride=2), :] = plane
            wide[p, pl.ds(1, half_rows, stride=2), :] = plane
        for p in range(px + 2 * HALO):
            low, own, high = wide[p, pl.ds(0, 8), :], wide[p, pl.ds(8, cy), :], wide[p, pl.ds(8 + cy, 8), :]
            if HALO <= p < HALO + px:
                black[p, own_rows, :] = mid[p, own_rows, :] + own
                black[p, low_rows, :] = jnp.where(sub == 7, mid[p, low_rows, :], landed[p, low_rows, :]) + low
                black[p, high_rows, :] = jnp.where(sub == 0, mid[p, high_rows, :], landed[p, high_rows, :]) + high
            else:
                black[p, own_rows, :] = landed[p, own_rows, :] + own
                black[p, low_rows, :] = landed[p, low_rows, :] + low
                black[p, high_rows, :] = landed[p, high_rows, :] + high
            if 1 <= p < px + 2 * HALO - 1:
                red[p, own_rows, :] = red[p, own_rows, :] + own
                red[p, low_rows, :] = red[p, low_rows, :] + low
                red[p, high_rows, :] = red[p, high_rows, :] + high

    with phase("post"):
        half_sweep(0, mix, red, black, red)
        half_sweep(1, black_rhs, black, red, black)
        half_sweep(2, mix, red, black, red)
        half_sweep(3, black_rhs, black, red, black, defect)

    with phase("last"):
        for first in range(0, px, 4):
            for a, centre, res in red_defects(black, range(first, first + 4)):
                value = black[HALO + a, own_rows, :]
                other = defect[a, pl.ds(REACH, cy), :]
                smoothed_ref[2 * a] = jnp.where(own_mask, centre, value)
                smoothed_ref[2 * a + 1] = jnp.where(own_mask, value, centre)
                residual_ref[2 * a] = jnp.where(own_mask, res, other)
                residual_ref[2 * a + 1] = jnp.where(own_mask, other, res)

    with phase("w_sent"):
        sent(second_coarse)
        sent(second_fine)
        sum_total(member_sums, 0, members).wait_send()
        sum_total(group_sums, 2, groups).wait_send()


def put(smoothed, residual, smoothed_out, residual_out, sem):
    copies = [
        pltpu.make_async_copy(smoothed, smoothed_out, sem.at[0]),
        pltpu.make_async_copy(residual, residual_out, sem.at[1]),
    ]
    for c in copies:
        c.start()
    for c in copies:
        c.wait()


def per_device(dims, source, potential, refined):
    cx, cy, cz = source.shape
    groups, members = dims
    px, hx, hy = cx // 2, cx // 4, cy // 2
    fine = (px + 2 * HALO, ROW0 + cy + ROW0, cz)
    coarse = (hx + 2 * CPLANE0, hy + 2 * CROW0, cz)
    f32 = jnp.float32
    dma = pltpu.SemaphoreType.DMA
    any_spec = pl.BlockSpec(memory_space=pl.ANY)
    vmem_spec = pl.BlockSpec(memory_space=pltpu.VMEM)
    most = max((2 * HALO + 1) * cy, (3 * REACH) * px) + 8
    results = pl.pallas_call(
        functools.partial(kernel, dims, (cx, cy, cz)),
        out_shape=[pltpu.VMEM(source.shape, f32)] * 2,
        in_specs=[pl.BlockSpec(memory_space=pltpu.SMEM), any_spec, any_spec],
        out_specs=[vmem_spec] * 2,
        scratch_shapes=[
            pltpu.VMEM((2, cx, cy, cz), f32),
            pltpu.VMEM((3, *fine), f32),
            pltpu.VMEM((px, cy, cz), f32),
            pltpu.VMEM(fine, f32),
            pltpu.VMEM(fine, f32),
            pltpu.VMEM(fine, f32),
            pltpu.VMEM((px, cy + 2 * REACH, cz), f32),
            pltpu.VMEM((px, cy, cz), f32),
            pltpu.VMEM(coarse, f32),
            pltpu.VMEM(coarse, f32),
            pltpu.VMEM(coarse, f32),
            pltpu.VMEM(coarse, f32),
            pltpu.VMEM(coarse, f32),
            pltpu.VMEM((px + 2 * HALO, cy + 16, cz), f32),
            pltpu.VMEM((3, 3, 8, cz), f32),
            pltpu.VMEM((3, cy + 2 * REACH, cz), f32),
            pltpu.VMEM((3, hy + 16, cz), f32),
            pltpu.VMEM((members, 8, cz), f32),
            pltpu.VMEM((groups, 8, cz), f32),
            pltpu.VMEM((most, cz), f32),
            dma((2,)),
            dma((3, len(SIDES))),
            dma((3, len(SIDES))),
            dma((4,)),
        ],
        compiler_params=pltpu.CompilerParams(collective_id=0, has_side_effects=True),
    )(refined, source, potential)
    return tuple(pl.pallas_call(
        put,
        out_shape=[jax.ShapeDtypeStruct(source.shape, f32)] * 2,
        in_specs=[any_spec] * 2,
        out_specs=[any_spec] * 2,
        scratch_shapes=[dma((2,))],
    )(*(pltpu.with_memory_space_constraint(v, pltpu.VMEM) for v in results)))


def solution(mesh):
    spec = P("group", "member", None)
    return jax.shard_map(
        functools.partial(per_device, (mesh.shape["group"], mesh.shape["member"])),
        mesh=mesh,
        in_specs=(spec, spec, spec),
        out_specs=(spec, spec),
        check_vma=False,
    )
```

```python
import contextlib
import functools

import jax
import jax.numpy as jnp
from jax import lax
from jax.experimental import pallas as pl
from jax.experimental.pallas import tpu as pltpu
from jax.sharding import PartitionSpec as P

SWEEPS = 2
COARSE = 2
REACH = 2 * SWEEPS
HALO = (REACH + 2) // 2
COARSE_REACH = 2 * COARSE - 1 + (REACH + 2) // 2
COARSE_HALO = COARSE_REACH // 2
ROW0 = 8 + REACH
CROW0 = 16
CPLANE0 = COARSE_HALO + 1
SIDES = ((0, -1), (0, 1), (-1, 0), (1, 0), (-1, -1), (-1, 1), (1, -1), (1, 1))
MESH = pl.DeviceIdType.MESH
SIXTH = 1.0 / 6.0
PIECES = 4


def phase(name):
    return contextlib.nullcontext()


def span(side, begin, end, first, count):
    if side == 0:
        return pl.ds(first, count), pl.ds(first, count)
    if side > 0:
        return pl.ds(first + count - end, end - begin), pl.ds(first - end, end - begin)
    return pl.ds(first + begin, end - begin), pl.ds(first + count + begin, end - begin)


def checker(rows, cz, lanes_per=1):
    r = lax.broadcasted_iota(jnp.int32, (rows, cz), 0)
    return ((r + lax.broadcasted_iota(jnp.int32, (rows, cz), 1) // lanes_per) & 1) == 0


def lanes(value, step):
    cz = value.shape[1]
    lane = lax.broadcasted_iota(jnp.int32, value.shape, 1)
    low = jnp.where(lane < step, 0.0, pltpu.roll(value, step, 1))
    high = jnp.where(lane >= cz - step, 0.0, pltpu.roll(value, cz - step, 1))
    return low + high


def neighbours(other, planes, row, rows, colour, mask, step):
    centres = {}
    out = []
    for p in planes:
        for q in (p - 1, p, p + 1):
            if q not in centres:
                centres[q] = other[q, pl.ds(row, rows), :]
        near, far = (centres[p - 1], centres[p + 1]) if colour == 0 else (centres[p + 1], centres[p - 1])
        total = centres[p] + jnp.where(mask, near, far)
        total = total + (other[p, pl.ds(row - 1, rows), :] + other[p, pl.ds(row + 1, rows), :])
        out.append(total + lanes(centres[p], step))
    return out


def kernel(
    dims, sizes,
    refined_hbm, source_ref, potential_ref,
    red, post, defect, own_rhs,
    refined_ref, raw, field, mid, landed, pair_rows, mixed, rhs0, rhs1, corr0, corr1, wide,
    flags, active, inside, member_sums, group_sums, zeros, dummy,
    local_sem, send_sem, recv_sem, sum_sem,
):
    groups, members = dims
    cx, cy, cz = sizes
    px, hx, hy = cx // 2, cx // 4, cy // 2
    group_at = lax.axis_index("group")
    member_at = lax.axis_index("member")
    f32 = jnp.float32
    black, mix, black_rhs = field.at[0], field.at[1], field.at[2]
    own_rows = pl.ds(ROW0, cy)
    window = cy + 2 * REACH
    cwindow = hy + 16

    load_source = pltpu.make_async_copy(source_ref, raw.at[0], local_sem.at[0])
    load_potential = pltpu.make_async_copy(potential_ref, raw.at[1], local_sem.at[1])
    load_refined = pltpu.make_async_copy(refined_hbm, refined_ref, local_sem.at[2])
    load_source.start()
    load_potential.start()
    load_refined.start()

    def there(dx, dy):
        ok = None
        for side, at, count in ((dx, group_at, groups), (dy, member_at, members)):
            if side == 0:
                continue
            here = at > 0 if side < 0 else at < count - 1
            ok = here if ok is None else ok & here
        return ok

    def device(dx, dy):
        return (group_at + dx, member_at + dy)

    barrier = pltpu.get_barrier_semaphore()
    for o in range(1, members):
        pl.semaphore_signal(barrier, inc=1, device_id=(group_at, lax.rem(member_at + o, members)), device_id_type=MESH)
    for o in range(1, groups):
        pl.semaphore_signal(barrier, inc=1, device_id=(lax.rem(group_at + o, groups), member_at), device_id_type=MESH)
    expected = jnp.int32(groups - 1 + members - 1)
    for dx, dy in SIDES:
        if dx and dy:
            @pl.when(there(dx, dy))
            def _():
                pl.semaphore_signal(barrier, inc=1, device_id=device(dx, dy), device_id_type=MESH)
            expected = expected + there(dx, dy).astype(jnp.int32)

    blank_rows = jnp.zeros((cy, cz), f32)
    for kind in range(2):
        for p in range(px):
            zeros[kind, p] = blank_rows
    blank_coarse = jnp.zeros((cwindow, cz), f32)
    for a in range(hx + 2 * CPLANE0):
        mixed[a, pl.ds(CROW0 - 8, cwindow), :] = blank_coarse
    for a in (0, hx + 2 * CPLANE0 - 1):
        corr0[a, pl.ds(CROW0 - 8, cwindow), :] = blank_coarse

    crow = lax.broadcasted_iota(jnp.int32, (cwindow, cz), 0) - 8
    clow = jnp.where(member_at > 0, -8, 0)
    chigh = jnp.where(member_at < members - 1, hy + 8, hy)
    within = jnp.where((crow >= clow) & (crow < chigh), SIXTH, 0.0)
    for region in range(3):
        alive = 1.0 if region == 1 else there(region - 1, 0).astype(f32)
        inside[region] = within * alive

    def wide_mask(rows):
        return lax.broadcasted_iota(jnp.int32, (rows, cz), 1) % 2 == 0

    with phase("load"):
        load_refined.wait()
        lane1 = lax.broadcasted_iota(jnp.int32, (1, cz), 1)
        boxes = refined_ref.shape[2]
        box = cz // boxes
        marks = jnp.zeros((1, cz), jnp.int32)
        for b in range(boxes):
            marks = jnp.where(lane1 // box == b, jnp.full((1, cz), refined_ref[0, 0, b], jnp.int32), marks)
        flags[1, 1, pl.ds(0, 1), :] = (marks == 1).astype(f32)
        load_source.wait()
        load_potential.wait()

    with phase("pack"):
        here = checker(cy, cz)
        smooth_own = jnp.broadcast_to(flags[1, 1, 0:1, :], (cy, cz)) > 0.5
        acc = [jnp.zeros((8, cz), f32)] * 4
        for a in range(px):
            s0, s1 = raw[0, 2 * a], raw[0, 2 * a + 1]
            v0, v1 = raw[1, 2 * a], raw[1, 2 * a + 1]
            both = s0 + s1
            acc = [acc[t] + sum(both[8 * u:8 * u + 8] for u in range(t, cy // 8, 4)) for t in range(4)]
            red_rhs = jnp.where(here, s0, s1)
            own_rhs[a] = red_rhs
            mix[HALO + a, own_rows, :] = jnp.where(smooth_own, red_rhs, jnp.where(here, v0, v1))
            black[HALO + a, own_rows, :] = jnp.where(here, v1, v0)
            black_rhs[HALO + a, own_rows, :] = jnp.where(here, s1, s0)
        acc = (acc[0] + acc[1]) + (acc[2] + acc[3])
        member_sums[0, pl.ds(0, 1), :] = jnp.sum(acc, axis=0, keepdims=True)

    with phase("barrier"):
        pl.semaphore_wait(barrier, expected)

    row = pl.ds(0, 1)

    def sum_copies(slots, n, count, target):
        return [
            pltpu.make_async_remote_copy(
                src_ref=slots.at[0, row], dst_ref=slots.at[o, row], send_sem=sum_sem.at[n], recv_sem=sum_sem.at[n + 1],
                device_id=target(o), device_id_type=MESH,
            )
            for o in range(1, count)
        ]

    def sum_total(slots, n, count):
        others = slots.at[pl.ds(1, count - 1), row]
        return pltpu.make_async_remote_copy(
            src_ref=others, dst_ref=others, send_sem=sum_sem.at[n], recv_sem=sum_sem.at[n + 1],
            device_id=(group_at, member_at), device_id_type=MESH,
        )

    def next_member(o):
        return (group_at, lax.rem(member_at + o, members))

    def next_group(o):
        return (lax.rem(group_at + o, groups), member_at)

    def first_round(n):
        dx, dy = SIDES[n]
        pairs = [(flags.at[1, 1, row], flags.at[1 - dx, 1 - dy, row])]
        if dx and dy:
            pieces = ((0, 1, 0, 1, 4), (1, 1, 0, 1, 3), (2, 1, 0, 1, 2), (0, 1, 1, 2, 2), (1, 1, 1, 2, 1))
        elif dx:
            pieces = ((0, 1, 0, HALO, cy), (1, 2, 0, HALO - 1, cy))
        else:
            pieces = ((0, 1, 0, px, REACH + 1), (1, 1, 0, px, REACH), (2, 1, 0, px, REACH - 1))
        for kind, kinds, begin, end, deep in pieces:
            sx, tx = span(dx, begin, end, HALO, px)
            sy, ty = span(dy, 0, deep, ROW0, cy)
            pairs.append((field.at[pl.ds(kind, kinds), sx, sy], field.at[pl.ds(kind, kinds), tx, ty]))
        return 0, pairs

    def second_coarse(n):
        dx, dy = SIDES[n]
        if dx and dy:
            pieces = ((0, 1, 5), (1, 2, 3), (2, 3, 1))
        elif dx:
            pieces = ((0, COARSE_HALO, hy),)
        else:
            pieces = ((0, hx, COARSE_REACH),)
        pairs = []
        for begin, end, deep in pieces:
            sx, tx = span(dx, begin, end, CPLANE0, hx)
            sy, ty = span(dy, 0, deep, CROW0, hy)
            pairs.append((mixed.at[sx, sy], mixed.at[tx, ty]))
        return 1, pairs

    def second_fine(n, early):
        dx, dy = SIDES[n]
        if dx and dy:
            pieces = () if early else ((0, 1, 0, 4), (1, 2, 0, 2))
        elif dx:
            pieces = () if early else ((0, HALO, 0, cy),)
        else:
            pieces = ((0, px // 2, 1, REACH + 1),) if early else ((px // 2, px, 1, REACH + 1),)
        pairs = []
        for begin, end, skip, deep in pieces:
            if dx:
                sx, tx = span(dx, begin, end, HALO, px)
            else:
                sx = tx = pl.ds(HALO + begin, end - begin)
            sy, ty = span(dy, skip, deep, ROW0, cy)
            pairs.append((mid.at[sx, sy], landed.at[tx, ty]))
        return 2, pairs

    early_fine = functools.partial(second_fine, early=True)
    late_fine = functools.partial(second_fine, early=False)

    def rows_of(pairs):
        total = 0
        for _, dst in pairs:
            total += functools.reduce(lambda p, q: p * q, dst.shape[:-1])
        return total

    def start(round_of):
        for n, (dx, dy) in enumerate(SIDES):
            kind, pairs = round_of(n)
            if not pairs:
                continue

            @pl.when(there(dx, dy))
            def _():
                for src, dst in pairs:
                    pltpu.make_async_remote_copy(
                        src_ref=src, dst_ref=dst, send_sem=send_sem.at[n], recv_sem=recv_sem.at[kind],
                        device_id=device(dx, dy), device_id_type=MESH,
                    ).start()

    def fill(round_of):
        for n, (dx, dy) in enumerate(SIDES):
            kind, pairs = round_of(n)
            if not pairs:
                continue

            @pl.when(jnp.logical_not(there(-dx, -dy)))
            def _():
                for _, dst in pairs:
                    shape = dst.shape[:-1]
                    src = zeros.at[(0,) * (4 - len(dst.shape)) + tuple(pl.ds(0, size) for size in shape)]
                    pltpu.make_async_copy(src, dst, recv_sem.at[kind]).start()

    def all_of(rows, n, kind):
        part = dummy.at[pl.ds(0, rows)]
        return pltpu.make_async_remote_copy(
            src_ref=part, dst_ref=part, send_sem=send_sem.at[n], recv_sem=recv_sem.at[kind],
            device_id=(group_at, member_at), device_id_type=MESH,
        )

    def arrive(*rounds):
        rows, kind = 0, None
        for round_of in rounds:
            for n in range(len(SIDES)):
                kind, pairs = round_of(n)
                rows += rows_of(pairs)
        all_of(rows, 0, kind).wait_recv()

    def sent(*rounds):
        for n, (dx, dy) in enumerate(SIDES):
            rows = sum(rows_of(round_of(n)[1]) for round_of in rounds)

            @pl.when(there(dx, dy))
            def _():
                all_of(rows, n, 0).wait_send()

    with phase("start1"):
        for c in sum_copies(member_sums, 0, members, next_member):
            c.start()
        start(first_round)
        fill(first_round)
        fill(second_coarse)
        fill(early_fine)
        fill(late_fine)

    with phase("w_msum"):
        sum_total(member_sums, 0, members).wait_recv()
    part = member_sums[0, row, :]
    for o in range(1, members):
        part = part + member_sums[o, row, :]
    group_sums[0, row, :] = part
    for c in sum_copies(group_sums, 2, groups, next_group):
        c.start()
    with phase("w_gsum"):
        sum_total(group_sums, 2, groups).wait_recv()
    with phase("mean"):
        total = group_sums[0, row, :]
        for o in range(1, groups):
            total = total + group_sums[o, row, :]
        mean = jnp.sum(total) / (cx * cy * cz * groups * members)
    with phase("w_halo1"):
        arrive(first_round)

    with phase("masks"):
        edge = lax.broadcasted_iota(jnp.int32, (8, cz), 0) < REACH
        for x in range(3):
            low, own, high = flags[x, 0], flags[x, 1], flags[x, 2]
            low, own, high = (jnp.broadcast_to(v[0:1], (8, cz)) for v in (low, own, high))
            active[x, pl.ds(0, 8), :] = jnp.where(edge, low, own)
            for t in range(1, window // 8 - 1):
                active[x, pl.ds(8 * t, 8), :] = own
            active[x, pl.ds(window - 8, 8), :] = jnp.where(edge, own, high)

    fine_mask = checker(window, cz)

    def half_sweep(t, right, old, other, out, also=None):
        colour = t % 2
        wide_by = (REACH - t + 1) // 2
        rows = pl.ds(ROW0 - REACH, window)
        for region, low, high in ((0, HALO - wide_by, HALO), (1, HALO, HALO + px), (2, HALO + px, HALO + px + wide_by)):
            keep = active[region] > 0.5
            for first in range(low, high, 4):
                planes = range(first, min(first + 4, high))
                sums = neighbours(other, planes, ROW0 - REACH, window, colour, fine_mask, 1)
                for p, nbr in zip(planes, sums):
                    total = right[p, rows, :] - mean + nbr
                    before = old[p, rows, :]
                    out[p, rows, :] = jnp.where(keep, total * SIXTH, before)
                    if also is not None and region == 1:
                        also[p - HALO] = jnp.where(keep, 0.0, total - 6.0 * before)

    with phase("pre"):
        half_sweep(0, mix, mix, black, red)
        half_sweep(1, black_rhs, black, red, mid)
        half_sweep(2, mix, mix, mid, red)
        half_sweep(3, black_rhs, black, red, mid, defect)

    own_mask = checker(cy, cz)

    def red_defects(other, planes):
        sums = neighbours(other, [HALO + a for a in planes], ROW0, cy, 0, own_mask, 1)
        for a, nbr in zip(planes, sums):
            centre = red[HALO + a, own_rows, :]
            yield a, centre, own_rhs[a] - mean + nbr - 6.0 * centre

    with phase("start_early"):
        start(early_fine)

    with phase("restrict"):
        for first in range(0, px, 4):
            for a, centre, res in red_defects(mid, range(first, first + 4)):
                pair_rows[a] = res + defect[a, pl.ds(REACH, cy), :]
        chosen, even = checker(hy, cz, 2), wide_mask(hy)
        for a in range(hx):
            first, second = (
                pair_rows[2 * a + k, pl.ds(0, hy, stride=2), :] + pair_rows[2 * a + k, pl.ds(1, hy, stride=2), :]
                for k in range(2)
            )
            zero, one = jnp.where(chosen, first, second), jnp.where(chosen, second, first)
            both = jnp.where(even, zero + pltpu.roll(zero, cz - 1, 1), one + pltpu.roll(one, 1, 1))
            mixed[CPLANE0 + a, pl.ds(CROW0, hy), :] = 0.5 * both

    with phase("start2"):
        start(second_coarse)
        start(late_fine)
        for a in range(px):
            own_rhs[a] = own_rhs[a] - mean
    with phase("w_coarse"):
        arrive(second_coarse)

    with phase("coarse"):
        coarse_rows = pl.ds(CROW0 - 8, cwindow)
        coarse_even = wide_mask(cwindow)
        coarse_mask = checker(cwindow, cz, 2)

        def regions(wide_by):
            first, last = CPLANE0, CPLANE0 + hx
            return (0, first - wide_by, first), (1, first, last), (2, last, last + wide_by)

        for region, low, high in regions(COARSE_HALO):
            weight = inside[region]
            for a in range(low, high):
                both = mixed[a, coarse_rows, :]
                s0 = jnp.where(coarse_even, both, pltpu.roll(both, 1, 1))
                rhs0[a, coarse_rows, :] = s0
                rhs1[a, coarse_rows, :] = jnp.where(coarse_even, pltpu.roll(both, cz - 1, 1), both)
                corr0[a, coarse_rows, :] = s0 * weight
        for t in range(1, 2 * COARSE):
            right, other, out = (rhs1, corr0, corr1) if t % 2 else (rhs0, corr1, corr0)
            for region, low, high in regions((COARSE_REACH - t + 1) // 2):
                weight = inside[region]
                for first in range(low, high, 4):
                    planes = range(first, min(first + 4, high))
                    sums = neighbours(other, planes, CROW0 - 8, cwindow, t % 2, coarse_mask, 2)
                    for a, nbr in zip(planes, sums):
                        out[a, coarse_rows, :] = (right[a, coarse_rows, :] + nbr) * weight

    with phase("w_fine2"):
        arrive(early_fine, late_fine)

    with phase("prolong"):
        half_rows = hy + 8
        rows = pl.ds(CROW0 - 4, half_rows)
        pick = checker(half_rows, cz, 2)
        low_rows, high_rows = pl.ds(ROW0 - 8, 8), pl.ds(ROW0 + cy, 8)
        sub = lax.broadcasted_iota(jnp.int32, (8, cz), 0)
        for p in range(px + 2 * HALO):
            a, k = CPLANE0 + (p - HALO) // 2, (p - HALO) % 2
            c0, c1 = corr0[a, rows, :], corr1[a, rows, :]
            plane = jnp.where(pick, c1, c0) if k else jnp.where(pick, c0, c1)
            wide[p, pl.ds(0, half_rows, stride=2), :] = plane
            wide[p, pl.ds(1, half_rows, stride=2), :] = plane
        for p in range(px + 2 * HALO):
            low, own, high = wide[p, pl.ds(0, 8), :], wide[p, pl.ds(8, cy), :], wide[p, pl.ds(8 + cy, 8), :]
            if HALO <= p < HALO + px:
                post[p, own_rows, :] = mid[p, own_rows, :] + own
                post[p, low_rows, :] = jnp.where(sub == 7, mid[p, low_rows, :], landed[p, low_rows, :]) + low
                post[p, high_rows, :] = jnp.where(sub == 0, mid[p, high_rows, :], landed[p, high_rows, :]) + high
            else:
                post[p, own_rows, :] = landed[p, own_rows, :] + own
                post[p, low_rows, :] = landed[p, low_rows, :] + low
                post[p, high_rows, :] = landed[p, high_rows, :] + high
            if 1 <= p < px + 2 * HALO - 1:
                red[p, own_rows, :] = red[p, own_rows, :] + own
                red[p, low_rows, :] = red[p, low_rows, :] + low
                red[p, high_rows, :] = red[p, high_rows, :] + high

    with phase("post"):
        half_sweep(0, mix, red, post, red)
        half_sweep(1, black_rhs, post, red, post)
        half_sweep(2, mix, red, post, red)
        half_sweep(3, black_rhs, post, red, post, defect)

    with phase("w_sent"):
        sent(first_round, second_coarse, early_fine, late_fine)
        sum_total(member_sums, 0, members).wait_send()
        sum_total(group_sums, 2, groups).wait_send()


def put(red, post, defect, contrast, smoothed_out, residual_out, smoothed, residual, sem):
    px, cy, cz = contrast.shape
    own_rows = pl.ds(ROW0, cy)
    mask = checker(cy, cz)
    size = px // PIECES
    copies = []
    for piece in range(PIECES):
        planes = range(piece * size, (piece + 1) * size)
        part = pl.ds(2 * piece * size, 2 * size)
        for a in planes:
            centre, value = red[HALO + a, own_rows, :], post[HALO + a, own_rows, :]
            smoothed[2 * a] = jnp.where(mask, centre, value)
            smoothed[2 * a + 1] = jnp.where(mask, value, centre)
        copies.append(pltpu.make_async_copy(smoothed.at[part], smoothed_out.at[part], sem.at[0, piece]))
        copies[-1].start()
        sums = neighbours(post, [HALO + a for a in planes], ROW0, cy, 0, mask, 1)
        for a, nbr in zip(planes, sums):
            res, other = contrast[a] + nbr - 6.0 * red[HALO + a, own_rows, :], defect[a, pl.ds(REACH, cy), :]
            residual[2 * a] = jnp.where(mask, res, other)
            residual[2 * a + 1] = jnp.where(mask, other, res)
        copies.append(pltpu.make_async_copy(residual.at[part], residual_out.at[part], sem.at[1, piece]))
        copies[-1].start()
    for c in copies:
        c.wait()


def per_device(dims, source, potential, refined):
    cx, cy, cz = source.shape
    groups, members = dims
    px, hx, hy = cx // 2, cx // 4, cy // 2
    fine = (px + 2 * HALO, ROW0 + cy + ROW0, cz)
    coarse = (hx + 2 * CPLANE0, hy + 2 * CROW0, cz)
    f32 = jnp.float32
    dma = pltpu.SemaphoreType.DMA
    any_spec = pl.BlockSpec(memory_space=pl.ANY)
    vmem_spec = pl.BlockSpec(memory_space=pltpu.VMEM)
    results = pl.pallas_call(
        functools.partial(kernel, dims, (cx, cy, cz)),
        out_shape=[
            pltpu.VMEM(fine, f32),
            pltpu.VMEM(fine, f32),
            pltpu.VMEM((px, cy + 2 * REACH, cz), f32),
            pltpu.VMEM((px, cy, cz), f32),
        ],
        in_specs=[any_spec] * 3,
        out_specs=[vmem_spec] * 4,
        scratch_shapes=[
            pltpu.SMEM(refined.shape, jnp.int32),
            pltpu.VMEM((2, cx, cy, cz), f32),
            pltpu.VMEM((3, *fine), f32),
            pltpu.VMEM(fine, f32),
            pltpu.VMEM(fine, f32),
            pltpu.VMEM((px, cy, cz), f32),
            pltpu.VMEM(coarse, f32),
            pltpu.VMEM(coarse, f32),
            pltpu.VMEM(coarse, f32),
            pltpu.VMEM(coarse, f32),
            pltpu.VMEM(coarse, f32),
            pltpu.VMEM((px + 2 * HALO, cy + 16, cz), f32),
            pltpu.VMEM((3, 3, 8, cz), f32),
            pltpu.VMEM((3, cy + 2 * REACH, cz), f32),
            pltpu.VMEM((3, hy + 16, cz), f32),
            pltpu.VMEM((members, 8, cz), f32),
            pltpu.VMEM((groups, 8, cz), f32),
            pltpu.VMEM((2, px, cy, cz), f32),
            pltpu.VMEM((64 * cy, cz), f32),
            dma((3,)),
            dma((len(SIDES),)),
            dma((3,)),
            dma((4,)),
        ],
        compiler_params=pltpu.CompilerParams(collective_id=0, has_side_effects=True),
    )(refined, source, potential)
    return tuple(pl.pallas_call(
        put,
        out_shape=[jax.ShapeDtypeStruct(source.shape, f32)] * 2,
        in_specs=[vmem_spec] * 4,
        out_specs=[any_spec] * 2,
        scratch_shapes=[pltpu.VMEM(source.shape, f32), pltpu.VMEM(source.shape, f32), dma((2, PIECES))],
    )(*(pltpu.with_memory_space_constraint(v, pltpu.VMEM) for v in results)))


def solution(mesh):
    spec = P("group", "member", None)
    return jax.shard_map(
        functools.partial(per_device, (mesh.shape["group"], mesh.shape["member"])),
        mesh=mesh,
        in_specs=(spec, spec, spec),
        out_specs=(spec, spec),
        check_vma=False,
    )
```

```python
import contextlib
import functools

import jax
import jax.numpy as jnp
from jax import lax
from jax.experimental import pallas as pl
from jax.experimental.pallas import tpu as pltpu
from jax.sharding import PartitionSpec as P

SWEEPS = 2
COARSE = 2
REACH = 2 * SWEEPS
HALO = (REACH + 2) // 2
COARSE_REACH = 2 * COARSE - 1 + (REACH + 2) // 2
COARSE_HALO = COARSE_REACH // 2
ROW0 = 8 + REACH
CROW0 = 16
CPLANE0 = COARSE_HALO + 1
SIDES = ((0, -1), (0, 1), (-1, 0), (1, 0), (-1, -1), (-1, 1), (1, -1), (1, 1))
MESH = pl.DeviceIdType.MESH
SIXTH = 1.0 / 6.0
PIECES = 4


def phase(name):
    return contextlib.nullcontext()


def span(side, begin, end, first, count):
    if side == 0:
        return pl.ds(first, count), pl.ds(first, count)
    if side > 0:
        return pl.ds(first + count - end, end - begin), pl.ds(first - end, end - begin)
    return pl.ds(first + begin, end - begin), pl.ds(first + count + begin, end - begin)


def checker(rows, cz, lanes_per=1):
    r = lax.broadcasted_iota(jnp.int32, (rows, cz), 0)
    return ((r + lax.broadcasted_iota(jnp.int32, (rows, cz), 1) // lanes_per) & 1) == 0


def lanes(value, step):
    cz = value.shape[1]
    lane = lax.broadcasted_iota(jnp.int32, value.shape, 1)
    low = jnp.where(lane < step, 0.0, pltpu.roll(value, step, 1))
    high = jnp.where(lane >= cz - step, 0.0, pltpu.roll(value, cz - step, 1))
    return low + high


def neighbours(other, planes, row, rows, colour, mask, step):
    centres = {}
    out = []
    for p in planes:
        for q in (p - 1, p, p + 1):
            if q not in centres:
                centres[q] = other[q, pl.ds(row, rows), :]
        near, far = (centres[p - 1], centres[p + 1]) if colour == 0 else (centres[p + 1], centres[p - 1])
        total = centres[p] + jnp.where(mask, near, far)
        total = total + (other[p, pl.ds(row - 1, rows), :] + other[p, pl.ds(row + 1, rows), :])
        out.append(total + lanes(centres[p], step))
    return out


def kernel(
    dims, sizes,
    refined_hbm, source_ref, potential_ref,
    red, post, defect, own_rhs,
    refined_ref, raw, field, mid, landed, pair_rows, mixed, rhs0, rhs1, corr0, corr1, wide,
    flags, active, inside, member_sums, group_sums, direct, zeros, dummy,
    local_sem, send_sem, recv_sem, sum_sem, ready,
):
    groups, members = dims
    cx, cy, cz = sizes
    px, hx, hy = cx // 2, cx // 4, cy // 2
    group_at = lax.axis_index("group")
    member_at = lax.axis_index("member")
    f32 = jnp.float32
    black, mix, black_rhs = field.at[0], field.at[1], field.at[2]
    own_rows = pl.ds(ROW0, cy)
    window = cy + 2 * REACH
    cwindow = hy + 16

    load_source = pltpu.make_async_copy(source_ref, raw.at[0], local_sem.at[0])
    load_potential = pltpu.make_async_copy(potential_ref, raw.at[1], local_sem.at[1])
    load_refined = pltpu.make_async_copy(refined_hbm, refined_ref, local_sem.at[2])
    load_source.start()
    load_potential.start()
    load_refined.start()

    def there(dx, dy):
        ok = None
        for side, at, count in ((dx, group_at, groups), (dy, member_at, members)):
            if side == 0:
                continue
            here = at > 0 if side < 0 else at < count - 1
            ok = here if ok is None else ok & here
        return ok

    def device(dx, dy):
        return (group_at + dx, member_at + dy)

    def signal(sem, at):
        pl.semaphore_signal(sem, inc=1, device_id=at, device_id_type=MESH)

    barrier = pltpu.get_barrier_semaphore()
    for o in range(1, members):
        signal(barrier, (group_at, lax.rem(member_at + o, members)))
    expected = jnp.int32(members - 1) + group_at * members
    for dy in (-1, 0, 1):
        @pl.when(there(-1, dy))
        def _():
            signal(barrier, device(-1, dy))
        expected = expected + there(1, dy).astype(jnp.int32)

    def greet(o, carry):
        for m in range(members):
            signal(barrier, (group_at + o, m))
        return carry

    lax.fori_loop(1, groups - group_at, greet, 0)

    blank_rows = jnp.zeros((cy, cz), f32)
    for kind in range(2):
        for p in range(px):
            zeros[kind, p] = blank_rows
    blank_coarse = jnp.zeros((cwindow, cz), f32)
    for a in range(hx + 2 * CPLANE0):
        mixed[a, pl.ds(CROW0 - 8, cwindow), :] = blank_coarse
    for a in (0, hx + 2 * CPLANE0 - 1):
        corr0[a, pl.ds(CROW0 - 8, cwindow), :] = blank_coarse

    crow = lax.broadcasted_iota(jnp.int32, (cwindow, cz), 0) - 8
    clow = jnp.where(member_at > 0, -8, 0)
    chigh = jnp.where(member_at < members - 1, hy + 8, hy)
    within = jnp.where((crow >= clow) & (crow < chigh), SIXTH, 0.0)
    for region in range(3):
        alive = 1.0 if region == 1 else there(region - 1, 0).astype(f32)
        inside[region] = within * alive

    def wide_mask(rows):
        return lax.broadcasted_iota(jnp.int32, (rows, cz), 1) % 2 == 0

    with phase("load"):
        load_refined.wait()
        lane1 = lax.broadcasted_iota(jnp.int32, (1, cz), 1)
        boxes = refined_ref.shape[2]
        box = cz // boxes
        marks = jnp.zeros((1, cz), jnp.int32)
        for b in range(boxes):
            marks = jnp.where(lane1 // box == b, jnp.full((1, cz), refined_ref[0, 0, b], jnp.int32), marks)
        flags[1, 1, pl.ds(0, 1), :] = (marks == 1).astype(f32)
        load_source.wait()
        load_potential.wait()

    with phase("pack"):
        here = checker(cy, cz)
        smooth_own = jnp.broadcast_to(flags[1, 1, 0:1, :], (cy, cz)) > 0.5
        acc = [jnp.zeros((8, cz), f32)] * 4
        for a in range(px):
            s0, s1 = raw[0, 2 * a], raw[0, 2 * a + 1]
            v0, v1 = raw[1, 2 * a], raw[1, 2 * a + 1]
            both = s0 + s1
            acc = [acc[t] + sum(both[8 * u:8 * u + 8] for u in range(t, cy // 8, 4)) for t in range(4)]
            red_rhs = jnp.where(here, s0, s1)
            own_rhs[a] = red_rhs
            mix[HALO + a, own_rows, :] = jnp.where(smooth_own, red_rhs, jnp.where(here, v0, v1))
            black[HALO + a, own_rows, :] = jnp.where(here, v1, v0)
            black_rhs[HALO + a, own_rows, :] = jnp.where(here, s1, s0)
        acc = (acc[0] + acc[1]) + (acc[2] + acc[3])
        member_sums[0, pl.ds(0, 1), :] = jnp.sum(acc, axis=0, keepdims=True)

    with phase("barrier"):
        pl.semaphore_wait(barrier, expected)

    def report(g, carry):
        signal(ready, (g, member_at))
        return carry

    row = pl.ds(0, 1)

    def sum_copy(src, dst, n, at):
        return pltpu.make_async_remote_copy(
            src_ref=src, dst_ref=dst, send_sem=sum_sem.at[n], recv_sem=sum_sem.at[n + 1], device_id=at, device_id_type=MESH,
        )

    own_sum, plane_sum = member_sums.at[0, row], group_sums.at[0, row]
    no_sum = zeros.at[0, 0, row]

    def share_in_plane():
        for o in range(1, members):
            sum_copy(own_sum, member_sums.at[o, row], 0, (group_at, lax.rem(member_at + o, members))).start()

    def share_with_earlier():
        for o in range(groups - 1, 0, -1):
            @pl.when(group_at >= o)
            def _():
                for m in range(members):
                    sum_copy(own_sum, direct.at[o, pl.ds(member_at, 1)], 2, (group_at - o, m)).start()

    def fill_sums():
        for o in range(1, groups):
            @pl.when(group_at < o)
            def _():
                pltpu.make_async_copy(zeros.at[0, 0, pl.ds(0, members)], dummy.at[pl.ds(o * members, members)], sum_sem.at[2]).start()
                pltpu.make_async_copy(no_sum, group_sums.at[o, row], sum_sem.at[5]).start()

            @pl.when(group_at + o >= groups)
            def _():
                pltpu.make_async_copy(zeros.at[0, 0, pl.ds(0, members)], direct.at[o], sum_sem.at[3]).start()
                pltpu.make_async_copy(no_sum, dummy.at[pl.ds(groups * members + o, 1)], sum_sem.at[4]).start()

    def share_with_later():
        for o in range(1, groups):
            @pl.when(group_at + o < groups)
            def _():
                sum_copy(plane_sum, group_sums.at[o, row], 4, (group_at + o, member_at)).start()

    def sums(slots, n):
        return sum_copy(slots, slots, n, (group_at, member_at))

    in_plane = sums(member_sums.at[pl.ds(1, members - 1), row], 0)
    from_later = sums(direct.at[pl.ds(1, groups - 1)], 2)
    from_earlier = sums(group_sums.at[pl.ds(1, groups - 1), row], 4)

    def first_round(n):
        dx, dy = SIDES[n]
        pairs = [(flags.at[1, 1, row], flags.at[1 - dx, 1 - dy, row])]
        if dx and dy:
            pieces = ((0, 1, 0, 1, 4), (1, 1, 0, 1, 3), (2, 1, 0, 1, 2), (0, 1, 1, 2, 2), (1, 1, 1, 2, 1))
        elif dx:
            pieces = ((0, 1, 0, HALO, cy), (1, 2, 0, HALO - 1, cy))
        else:
            pieces = ((0, 1, 0, px, REACH + 1), (1, 1, 0, px, REACH), (2, 1, 0, px, REACH - 1))
        for kind, kinds, begin, end, deep in pieces:
            sx, tx = span(dx, begin, end, HALO, px)
            sy, ty = span(dy, 0, deep, ROW0, cy)
            pairs.append((field.at[pl.ds(kind, kinds), sx, sy], field.at[pl.ds(kind, kinds), tx, ty]))
        return 0, pairs

    def second_coarse(n):
        dx, dy = SIDES[n]
        if dx and dy:
            pieces = ((0, 1, 5), (1, 2, 3), (2, 3, 1))
        elif dx:
            pieces = ((0, COARSE_HALO, hy),)
        else:
            pieces = ((0, hx, COARSE_REACH),)
        pairs = []
        for begin, end, deep in pieces:
            sx, tx = span(dx, begin, end, CPLANE0, hx)
            sy, ty = span(dy, 0, deep, CROW0, hy)
            pairs.append((mixed.at[sx, sy], mixed.at[tx, ty]))
        return 1, pairs

    def second_fine(n, early):
        dx, dy = SIDES[n]
        if dx and dy:
            pieces = () if early else ((0, 1, 0, 4), (1, 2, 0, 2))
        elif dx:
            pieces = () if early else ((0, HALO, 0, cy),)
        else:
            pieces = ((0, px // 2, 1, REACH + 1),) if early else ((px // 2, px, 1, REACH + 1),)
        pairs = []
        for begin, end, skip, deep in pieces:
            if dx:
                sx, tx = span(dx, begin, end, HALO, px)
            else:
                sx = tx = pl.ds(HALO + begin, end - begin)
            sy, ty = span(dy, skip, deep, ROW0, cy)
            pairs.append((mid.at[sx, sy], landed.at[tx, ty]))
        return 2, pairs

    early_fine = functools.partial(second_fine, early=True)
    late_fine = functools.partial(second_fine, early=False)

    def rows_of(pairs):
        total = 0
        for _, dst in pairs:
            total += functools.reduce(lambda p, q: p * q, dst.shape[:-1])
        return total

    def start(round_of):
        for n, (dx, dy) in enumerate(SIDES):
            kind, pairs = round_of(n)
            if not pairs:
                continue

            @pl.when(there(dx, dy))
            def _():
                for src, dst in pairs:
                    pltpu.make_async_remote_copy(
                        src_ref=src, dst_ref=dst, send_sem=send_sem.at[n], recv_sem=recv_sem.at[kind],
                        device_id=device(dx, dy), device_id_type=MESH,
                    ).start()

    def fill(round_of):
        for n, (dx, dy) in enumerate(SIDES):
            kind, pairs = round_of(n)
            if not pairs:
                continue

            @pl.when(jnp.logical_not(there(-dx, -dy)))
            def _():
                for _, dst in pairs:
                    shape = dst.shape[:-1]
                    src = zeros.at[(0,) * (4 - len(dst.shape)) + tuple(pl.ds(0, size) for size in shape)]
                    pltpu.make_async_copy(src, dst, recv_sem.at[kind]).start()

    def all_of(rows, n, kind):
        part = dummy.at[pl.ds(0, rows)]
        return pltpu.make_async_remote_copy(
            src_ref=part, dst_ref=part, send_sem=send_sem.at[n], recv_sem=recv_sem.at[kind],
            device_id=(group_at, member_at), device_id_type=MESH,
        )

    def arrive(*rounds):
        rows, kind = 0, None
        for round_of in rounds:
            for n in range(len(SIDES)):
                kind, pairs = round_of(n)
                rows += rows_of(pairs)
        all_of(rows, 0, kind).wait_recv()

    def sent(*rounds):
        for n, (dx, dy) in enumerate(SIDES):
            rows = sum(rows_of(round_of(n)[1]) for round_of in rounds)

            @pl.when(there(dx, dy))
            def _():
                all_of(rows, n, 0).wait_send()

    with phase("start1"):
        share_in_plane()
        share_with_earlier()
        start(first_round)
        lax.fori_loop(0, group_at, report, 0)
    with phase("fill"):
        fill_sums()
        for round_of in (first_round, second_coarse, early_fine, late_fine):
            fill(round_of)

    with phase("w_msum"):
        in_plane.wait_recv()
    part = member_sums[0, row, :]
    for o in range(1, members):
        part = part + member_sums[o, row, :]
    group_sums[0, row, :] = part
    with phase("w_ready"):
        @pl.when(group_at < groups - 1)
        def _():
            pl.semaphore_wait(ready, groups - 1 - group_at)
    share_with_later()
    with phase("w_gsum"):
        from_earlier.wait_recv()
    with phase("w_direct"):
        from_later.wait_recv()
    with phase("mean"):
        total = group_sums[0, row, :]
        later = jnp.zeros((members, cz), f32)
        for o in range(1, groups):
            total = total + group_sums[o, row, :]
            later = later + direct[o]
        total = total + jnp.sum(later, axis=0, keepdims=True)
        mean = jnp.sum(total) / (cx * cy * cz * groups * members)
    with phase("w_halo1"):
        arrive(first_round)

    with phase("masks"):
        edge = lax.broadcasted_iota(jnp.int32, (8, cz), 0) < REACH
        for x in range(3):
            low, own, high = flags[x, 0], flags[x, 1], flags[x, 2]
            low, own, high = (jnp.broadcast_to(v[0:1], (8, cz)) for v in (low, own, high))
            active[x, pl.ds(0, 8), :] = jnp.where(edge, low, own)
            for t in range(1, window // 8 - 1):
                active[x, pl.ds(8 * t, 8), :] = own
            active[x, pl.ds(window - 8, 8), :] = jnp.where(edge, own, high)

    fine_mask = checker(window, cz)

    def half_sweep(t, right, old, other, out, also=None):
        colour = t % 2
        wide_by = (REACH - t + 1) // 2
        rows = pl.ds(ROW0 - REACH, window)
        for region, low, high in ((0, HALO - wide_by, HALO), (1, HALO, HALO + px), (2, HALO + px, HALO + px + wide_by)):
            keep = active[region] > 0.5
            for first in range(low, high, 4):
                planes = range(first, min(first + 4, high))
                sums = neighbours(other, planes, ROW0 - REACH, window, colour, fine_mask, 1)
                for p, nbr in zip(planes, sums):
                    total = right[p, rows, :] - mean + nbr
                    before = old[p, rows, :]
                    out[p, rows, :] = jnp.where(keep, total * SIXTH, before)
                    if also is not None and region == 1:
                        also[p - HALO] = jnp.where(keep, 0.0, total - 6.0 * before)

    with phase("pre"):
        half_sweep(0, mix, mix, black, red)
        half_sweep(1, black_rhs, black, red, mid)
        half_sweep(2, mix, mix, mid, red)
        half_sweep(3, black_rhs, black, red, mid, defect)

    own_mask = checker(cy, cz)

    def red_defects(other, planes):
        sums = neighbours(other, [HALO + a for a in planes], ROW0, cy, 0, own_mask, 1)
        for a, nbr in zip(planes, sums):
            centre = red[HALO + a, own_rows, :]
            yield a, centre, own_rhs[a] - mean + nbr - 6.0 * centre

    with phase("start_early"):
        start(early_fine)

    with phase("restrict"):
        for first in range(0, px, 4):
            for a, centre, res in red_defects(mid, range(first, first + 4)):
                pair_rows[a] = res + defect[a, pl.ds(REACH, cy), :]
        chosen, even = checker(hy, cz, 2), wide_mask(hy)
        for a in range(hx):
            first, second = (
                pair_rows[2 * a + k, pl.ds(0, hy, stride=2), :] + pair_rows[2 * a + k, pl.ds(1, hy, stride=2), :]
                for k in range(2)
            )
            zero, one = jnp.where(chosen, first, second), jnp.where(chosen, second, first)
            both = jnp.where(even, zero + pltpu.roll(zero, cz - 1, 1), one + pltpu.roll(one, 1, 1))
            mixed[CPLANE0 + a, pl.ds(CROW0, hy), :] = 0.5 * both

    with phase("start2"):
        start(second_coarse)
        start(late_fine)
        for a in range(px):
            own_rhs[a] = own_rhs[a] - mean
    with phase("w_coarse"):
        arrive(second_coarse)

    with phase("coarse"):
        coarse_rows = pl.ds(CROW0 - 8, cwindow)
        coarse_even = wide_mask(cwindow)
        coarse_mask = checker(cwindow, cz, 2)

        def regions(wide_by):
            first, last = CPLANE0, CPLANE0 + hx
            return (0, first - wide_by, first), (1, first, last), (2, last, last + wide_by)

        for region, low, high in regions(COARSE_HALO):
            weight = inside[region]
            for a in range(low, high):
                both = mixed[a, coarse_rows, :]
                s0 = jnp.where(coarse_even, both, pltpu.roll(both, 1, 1))
                rhs0[a, coarse_rows, :] = s0
                rhs1[a, coarse_rows, :] = jnp.where(coarse_even, pltpu.roll(both, cz - 1, 1), both)
                corr0[a, coarse_rows, :] = s0 * weight
        for t in range(1, 2 * COARSE):
            right, other, out = (rhs1, corr0, corr1) if t % 2 else (rhs0, corr1, corr0)
            for region, low, high in regions((COARSE_REACH - t + 1) // 2):
                weight = inside[region]
                for first in range(low, high, 4):
                    planes = range(first, min(first + 4, high))
                    sums = neighbours(other, planes, CROW0 - 8, cwindow, t % 2, coarse_mask, 2)
                    for a, nbr in zip(planes, sums):
                        out[a, coarse_rows, :] = (right[a, coarse_rows, :] + nbr) * weight

    with phase("w_fine2"):
        arrive(early_fine, late_fine)

    with phase("prolong"):
        half_rows = hy + 8
        rows = pl.ds(CROW0 - 4, half_rows)
        pick = checker(half_rows, cz, 2)
        low_rows, high_rows = pl.ds(ROW0 - 8, 8), pl.ds(ROW0 + cy, 8)
        sub = lax.broadcasted_iota(jnp.int32, (8, cz), 0)
        for p in range(px + 2 * HALO):
            a, k = CPLANE0 + (p - HALO) // 2, (p - HALO) % 2
            c0, c1 = corr0[a, rows, :], corr1[a, rows, :]
            plane = jnp.where(pick, c1, c0) if k else jnp.where(pick, c0, c1)
            wide[p, pl.ds(0, half_rows, stride=2), :] = plane
            wide[p, pl.ds(1, half_rows, stride=2), :] = plane
        for p in range(px + 2 * HALO):
            low, own, high = wide[p, pl.ds(0, 8), :], wide[p, pl.ds(8, cy), :], wide[p, pl.ds(8 + cy, 8), :]
            if HALO <= p < HALO + px:
                post[p, own_rows, :] = mid[p, own_rows, :] + own
                post[p, low_rows, :] = jnp.where(sub == 7, mid[p, low_rows, :], landed[p, low_rows, :]) + low
                post[p, high_rows, :] = jnp.where(sub == 0, mid[p, high_rows, :], landed[p, high_rows, :]) + high
            else:
                post[p, own_rows, :] = landed[p, own_rows, :] + own
                post[p, low_rows, :] = landed[p, low_rows, :] + low
                post[p, high_rows, :] = landed[p, high_rows, :] + high
            if 1 <= p < px + 2 * HALO - 1:
                red[p, own_rows, :] = red[p, own_rows, :] + own
                red[p, low_rows, :] = red[p, low_rows, :] + low
                red[p, high_rows, :] = red[p, high_rows, :] + high

    with phase("post"):
        half_sweep(0, mix, red, post, red)
        half_sweep(1, black_rhs, post, red, post)
        half_sweep(2, mix, red, post, red)
        half_sweep(3, black_rhs, post, red, post, defect)

    with phase("w_sent"):
        sent(first_round, second_coarse, early_fine, late_fine)
        in_plane.wait_send()
        from_later.wait_send()
        from_earlier.wait_send()


def put(red, post, defect, contrast, smoothed_out, residual_out, smoothed, residual, sem):
    px, cy, cz = contrast.shape
    own_rows = pl.ds(ROW0, cy)
    mask = checker(cy, cz)
    size = px // PIECES
    copies = []
    for piece in range(PIECES):
        planes = range(piece * size, (piece + 1) * size)
        part = pl.ds(2 * piece * size, 2 * size)
        for a in planes:
            centre, value = red[HALO + a, own_rows, :], post[HALO + a, own_rows, :]
            smoothed[2 * a] = jnp.where(mask, centre, value)
            smoothed[2 * a + 1] = jnp.where(mask, value, centre)
        copies.append(pltpu.make_async_copy(smoothed.at[part], smoothed_out.at[part], sem.at[0, piece]))
        copies[-1].start()
        sums = neighbours(post, [HALO + a for a in planes], ROW0, cy, 0, mask, 1)
        for a, nbr in zip(planes, sums):
            res, other = contrast[a] + nbr - 6.0 * red[HALO + a, own_rows, :], defect[a, pl.ds(REACH, cy), :]
            residual[2 * a] = jnp.where(mask, res, other)
            residual[2 * a + 1] = jnp.where(mask, other, res)
        copies.append(pltpu.make_async_copy(residual.at[part], residual_out.at[part], sem.at[1, piece]))
        copies[-1].start()
    for c in copies:
        c.wait()


def per_device(dims, source, potential, refined):
    cx, cy, cz = source.shape
    groups, members = dims
    px, hx, hy = cx // 2, cx // 4, cy // 2
    fine = (px + 2 * HALO, ROW0 + cy + ROW0, cz)
    coarse = (hx + 2 * CPLANE0, hy + 2 * CROW0, cz)
    f32 = jnp.float32
    dma = pltpu.SemaphoreType.DMA
    any_spec = pl.BlockSpec(memory_space=pl.ANY)
    vmem_spec = pl.BlockSpec(memory_space=pltpu.VMEM)
    results = pl.pallas_call(
        functools.partial(kernel, dims, (cx, cy, cz)),
        out_shape=[
            pltpu.VMEM(fine, f32),
            pltpu.VMEM(fine, f32),
            pltpu.VMEM((px, cy + 2 * REACH, cz), f32),
            pltpu.VMEM((px, cy, cz), f32),
        ],
        in_specs=[any_spec] * 3,
        out_specs=[vmem_spec] * 4,
        scratch_shapes=[
            pltpu.SMEM(refined.shape, jnp.int32),
            pltpu.VMEM((2, cx, cy, cz), f32),
            pltpu.VMEM((3, *fine), f32),
            pltpu.VMEM(fine, f32),
            pltpu.VMEM(fine, f32),
            pltpu.VMEM((px, cy, cz), f32),
            pltpu.VMEM(coarse, f32),
            pltpu.VMEM(coarse, f32),
            pltpu.VMEM(coarse, f32),
            pltpu.VMEM(coarse, f32),
            pltpu.VMEM(coarse, f32),
            pltpu.VMEM((px + 2 * HALO, cy + 16, cz), f32),
            pltpu.VMEM((3, 3, 8, cz), f32),
            pltpu.VMEM((3, cy + 2 * REACH, cz), f32),
            pltpu.VMEM((3, hy + 16, cz), f32),
            pltpu.VMEM((members, 8, cz), f32),
            pltpu.VMEM((groups, 8, cz), f32),
            pltpu.VMEM((groups, members, cz), f32),
            pltpu.VMEM((2, px, cy, cz), f32),
            pltpu.VMEM((64 * cy, cz), f32),
            dma((3,)),
            dma((len(SIDES),)),
            dma((3,)),
            dma((6,)),
            pltpu.SemaphoreType.REGULAR,
        ],
        compiler_params=pltpu.CompilerParams(collective_id=0, has_side_effects=True),
    )(refined, source, potential)
    return tuple(pl.pallas_call(
        put,
        out_shape=[jax.ShapeDtypeStruct(source.shape, f32)] * 2,
        in_specs=[vmem_spec] * 4,
        out_specs=[any_spec] * 2,
        scratch_shapes=[pltpu.VMEM(source.shape, f32), pltpu.VMEM(source.shape, f32), dma((2, PIECES))],
    )(*(pltpu.with_memory_space_constraint(v, pltpu.VMEM) for v in results)))


def solution(mesh):
    spec = P("group", "member", None)
    return jax.shard_map(
        functools.partial(per_device, (mesh.shape["group"], mesh.shape["member"])),
        mesh=mesh,
        in_specs=(spec, spec, spec),
        out_specs=(spec, spec),
        check_vma=False,
    )
```

```python
import contextlib
import functools

import jax
import jax.numpy as jnp
from jax import lax
from jax.experimental import pallas as pl
from jax.experimental.pallas import tpu as pltpu
from jax.sharding import PartitionSpec as P

SWEEPS = 2
COARSE = 2
REACH = 2 * SWEEPS
HALO = (REACH + 2) // 2
COARSE_REACH = 2 * COARSE - 1 + (REACH + 2) // 2
COARSE_HALO = COARSE_REACH // 2
ROW0 = 8 + REACH
CROW0 = 16
CPLANE0 = COARSE_HALO + 1
SIDES = ((0, -1), (0, 1), (-1, 0), (1, 0), (-1, -1), (-1, 1), (1, -1), (1, 1))
MESH = pl.DeviceIdType.MESH
SIXTH = 1.0 / 6.0
PIECES = 4


def phase(name):
    return contextlib.nullcontext()


def span(side, begin, end, first, count):
    if side == 0:
        return pl.ds(first, count), pl.ds(first, count)
    if side > 0:
        return pl.ds(first + count - end, end - begin), pl.ds(first - end, end - begin)
    return pl.ds(first + begin, end - begin), pl.ds(first + count + begin, end - begin)


def checker(rows, cz, lanes_per=1):
    r = lax.broadcasted_iota(jnp.int32, (rows, cz), 0)
    return ((r + lax.broadcasted_iota(jnp.int32, (rows, cz), 1) // lanes_per) & 1) == 0


def lanes(value, step):
    cz = value.shape[1]
    lane = lax.broadcasted_iota(jnp.int32, value.shape, 1)
    low = jnp.where(lane < step, 0.0, pltpu.roll(value, step, 1))
    high = jnp.where(lane >= cz - step, 0.0, pltpu.roll(value, cz - step, 1))
    return low + high


def neighbours(other, planes, row, rows, colour, mask, step):
    centres = {}
    out = []
    for p in planes:
        for q in (p - 1, p, p + 1):
            if q not in centres:
                centres[q] = other[q, pl.ds(row, rows), :]
        near, far = (centres[p - 1], centres[p + 1]) if colour == 0 else (centres[p + 1], centres[p - 1])
        total = centres[p] + jnp.where(mask, near, far)
        total = total + (other[p, pl.ds(row - 1, rows), :] + other[p, pl.ds(row + 1, rows), :])
        out.append(total + lanes(centres[p], step))
    return out


def kernel(
    dims, sizes,
    refined_hbm, source_ref, potential_ref,
    red, post, defect, own_rhs,
    refined_ref, raw, field, mid, landed, pair_rows, mixed, rhs0, rhs1, corr0, corr1, wide,
    flags, active, inside, member_sums, group_sums, direct, zeros, dummy,
    local_sem, send_sem, recv_sem, sum_sem, ready,
):
    groups, members = dims
    cx, cy, cz = sizes
    px, hx, hy = cx // 2, cx // 4, cy // 2
    group_at = lax.axis_index("group")
    member_at = lax.axis_index("member")
    f32 = jnp.float32
    black, mix, black_rhs = field.at[0], field.at[1], field.at[2]
    own_rows = pl.ds(ROW0, cy)
    window = cy + 2 * REACH
    cwindow = hy + 16

    load_source = pltpu.make_async_copy(source_ref, raw.at[0], local_sem.at[0])
    load_potential = pltpu.make_async_copy(potential_ref, raw.at[1], local_sem.at[1])
    load_refined = pltpu.make_async_copy(refined_hbm, refined_ref, local_sem.at[2])
    load_source.start()
    load_potential.start()
    load_refined.start()

    def there(dx, dy):
        ok = None
        for side, at, count in ((dx, group_at, groups), (dy, member_at, members)):
            if side == 0:
                continue
            here = at > 0 if side < 0 else at < count - 1
            ok = here if ok is None else ok & here
        return ok

    def device(dx, dy):
        return (group_at + dx, member_at + dy)

    def signal(sem, at):
        pl.semaphore_signal(sem, inc=1, device_id=at, device_id_type=MESH)

    barrier = pltpu.get_barrier_semaphore()
    for o in range(1, members):
        signal(barrier, (group_at, lax.rem(member_at + o, members)))
    expected = jnp.int32(members - 1) + group_at * members
    for dy in (-1, 0, 1):
        @pl.when(there(-1, dy))
        def _():
            signal(barrier, device(-1, dy))
        expected = expected + there(1, dy).astype(jnp.int32)

    def greet(o, carry):
        for m in range(members):
            signal(barrier, (group_at + o, m))
        return carry

    lax.fori_loop(1, groups - group_at, greet, 0)

    blank_rows = jnp.zeros((cy, cz), f32)
    for kind in range(2):
        for p in range(px):
            zeros[kind, p] = blank_rows
    blank_coarse = jnp.zeros((cwindow, cz), f32)
    for a in range(hx + 2 * CPLANE0):
        mixed[a, pl.ds(CROW0 - 8, cwindow), :] = blank_coarse
    for a in (0, hx + 2 * CPLANE0 - 1):
        corr0[a, pl.ds(CROW0 - 8, cwindow), :] = blank_coarse

    crow = lax.broadcasted_iota(jnp.int32, (cwindow, cz), 0) - 8
    clow = jnp.where(member_at > 0, -8, 0)
    chigh = jnp.where(member_at < members - 1, hy + 8, hy)
    within = jnp.where((crow >= clow) & (crow < chigh), SIXTH, 0.0)
    for region in range(3):
        alive = 1.0 if region == 1 else there(region - 1, 0).astype(f32)
        inside[region] = within * alive

    def wide_mask(rows):
        return lax.broadcasted_iota(jnp.int32, (rows, cz), 1) % 2 == 0

    with phase("load"):
        load_refined.wait()
        lane1 = lax.broadcasted_iota(jnp.int32, (1, cz), 1)
        boxes = refined_ref.shape[2]
        box = cz // boxes
        marks = jnp.zeros((1, cz), jnp.int32)
        for b in range(boxes):
            marks = jnp.where(lane1 // box == b, jnp.full((1, cz), refined_ref[0, 0, b], jnp.int32), marks)
        flags[1, 1, pl.ds(0, 1), :] = (marks == 1).astype(f32)
        load_source.wait()
        load_potential.wait()

    with phase("pack"):
        here = checker(cy, cz)
        smooth_own = jnp.broadcast_to(flags[1, 1, 0:1, :], (cy, cz)) > 0.5
        acc = [jnp.zeros((8, cz), f32)] * 4
        for a in range(px):
            s0, s1 = raw[0, 2 * a], raw[0, 2 * a + 1]
            v0, v1 = raw[1, 2 * a], raw[1, 2 * a + 1]
            both = s0 + s1
            acc = [acc[t] + sum(both[8 * u:8 * u + 8] for u in range(t, cy // 8, 4)) for t in range(4)]
            red_rhs = jnp.where(here, s0, s1)
            own_rhs[a] = red_rhs
            mix[HALO + a, own_rows, :] = jnp.where(smooth_own, red_rhs, jnp.where(here, v0, v1))
            black[HALO + a, own_rows, :] = jnp.where(here, v1, v0)
            black_rhs[HALO + a, own_rows, :] = jnp.where(here, s1, s0)
        acc = (acc[0] + acc[1]) + (acc[2] + acc[3])
        member_sums[0, pl.ds(0, 1), :] = jnp.sum(acc, axis=0, keepdims=True)

    with phase("barrier"):
        pl.semaphore_wait(barrier, expected)

    def report(g, carry):
        signal(ready, (g, member_at))
        return carry

    lax.fori_loop(0, group_at, report, 0)

    row = pl.ds(0, 1)

    def sum_copy(src, dst, n, at):
        return pltpu.make_async_remote_copy(
            src_ref=src, dst_ref=dst, send_sem=sum_sem.at[n], recv_sem=sum_sem.at[n + 1], device_id=at, device_id_type=MESH,
        )

    own_sum, plane_sum = member_sums.at[0, row], group_sums.at[0, row]
    no_sum = zeros.at[0, 0, row]

    def share_in_plane():
        for o in range(1, members):
            sum_copy(own_sum, member_sums.at[o, row], 0, (group_at, lax.rem(member_at + o, members))).start()

    def share_with_earlier():
        for o in range(groups - 1, 0, -1):
            @pl.when(group_at >= o)
            def _():
                for m in range(members):
                    sum_copy(own_sum, direct.at[o, pl.ds(member_at, 1)], 2, (group_at - o, m)).start()

    def fill_sums():
        for o in range(1, groups):
            @pl.when(group_at < o)
            def _():
                pltpu.make_async_copy(zeros.at[0, 0, pl.ds(0, members)], dummy.at[pl.ds(o * members, members)], sum_sem.at[2]).start()
                pltpu.make_async_copy(no_sum, group_sums.at[o, row], sum_sem.at[5]).start()

            @pl.when(group_at + o >= groups)
            def _():
                pltpu.make_async_copy(zeros.at[0, 0, pl.ds(0, members)], direct.at[o], sum_sem.at[3]).start()
                pltpu.make_async_copy(no_sum, dummy.at[pl.ds(groups * members + o, 1)], sum_sem.at[4]).start()

    def share_with_later():
        for o in range(1, groups):
            @pl.when(group_at + o < groups)
            def _():
                sum_copy(plane_sum, group_sums.at[o, row], 4, (group_at + o, member_at)).start()

    def sums(slots, n):
        return sum_copy(slots, slots, n, (group_at, member_at))

    in_plane = sums(member_sums.at[pl.ds(1, members - 1), row], 0)
    from_later = sums(direct.at[pl.ds(1, groups - 1)], 2)
    from_earlier = sums(group_sums.at[pl.ds(1, groups - 1), row], 4)

    def first_round(n):
        dx, dy = SIDES[n]
        pairs = [(flags.at[1, 1, row], flags.at[1 - dx, 1 - dy, row])]
        if dx and dy:
            pieces = ((0, 1, 0, 1, 4), (1, 1, 0, 1, 3), (2, 1, 0, 1, 2), (0, 1, 1, 2, 2), (1, 1, 1, 2, 1))
        elif dx:
            pieces = ((0, 1, 0, HALO, cy), (1, 2, 0, HALO - 1, cy))
        else:
            pieces = ((0, 1, 0, px, REACH + 1), (1, 1, 0, px, REACH), (2, 1, 0, px, REACH - 1))
        for kind, kinds, begin, end, deep in pieces:
            sx, tx = span(dx, begin, end, HALO, px)
            sy, ty = span(dy, 0, deep, ROW0, cy)
            pairs.append((field.at[pl.ds(kind, kinds), sx, sy], field.at[pl.ds(kind, kinds), tx, ty]))
        return 0, pairs

    def second_coarse(n):
        dx, dy = SIDES[n]
        if dx and dy:
            pieces = ((0, 1, 5), (1, 2, 3), (2, 3, 1))
        elif dx:
            pieces = ((0, COARSE_HALO, hy),)
        else:
            pieces = ((0, hx, COARSE_REACH),)
        pairs = []
        for begin, end, deep in pieces:
            sx, tx = span(dx, begin, end, CPLANE0, hx)
            sy, ty = span(dy, 0, deep, CROW0, hy)
            pairs.append((mixed.at[sx, sy], mixed.at[tx, ty]))
        return 1, pairs

    def second_fine(n):
        dx, dy = SIDES[n]
        if dx and dy:
            pieces = ((0, 1, 0, 4), (1, 2, 0, 2))
        elif dx:
            pieces = ((0, HALO, 0, cy),)
        else:
            pieces = ((0, px, 1, REACH + 1),)
        pairs = []
        for begin, end, skip, deep in pieces:
            sx, tx = span(dx, begin, end, HALO, px)
            sy, ty = span(dy, skip, deep, ROW0, cy)
            pairs.append((mid.at[sx, sy], landed.at[tx, ty]))
        return 2, pairs

    def rows_of(pairs):
        total = 0
        for _, dst in pairs:
            total += functools.reduce(lambda p, q: p * q, dst.shape[:-1])
        return total

    odd = lax.rem(member_at, 2) == 1

    def start(round_of):
        for far in (True, None, False):
            for n, (dx, dy) in enumerate(SIDES):
                if (dy == 0) != (far is None):
                    continue
                kind, pairs = round_of(n)
                now = there(dx, dy)
                if far is not None:
                    now = now & (odd if (dy > 0) == far else jnp.logical_not(odd))

                @pl.when(now)
                def _():
                    for src, dst in pairs:
                        pltpu.make_async_remote_copy(
                            src_ref=src, dst_ref=dst, send_sem=send_sem.at[n], recv_sem=recv_sem.at[kind],
                            device_id=device(dx, dy), device_id_type=MESH,
                        ).start()

    def fill(round_of):
        for n, (dx, dy) in enumerate(SIDES):
            kind, pairs = round_of(n)
            @pl.when(jnp.logical_not(there(-dx, -dy)))
            def _():
                for _, dst in pairs:
                    shape = dst.shape[:-1]
                    src = zeros.at[(0,) * (4 - len(dst.shape)) + tuple(pl.ds(0, size) for size in shape)]
                    pltpu.make_async_copy(src, dst, recv_sem.at[kind]).start()

    def all_of(rows, n, kind):
        part = dummy.at[pl.ds(0, rows)]
        return pltpu.make_async_remote_copy(
            src_ref=part, dst_ref=part, send_sem=send_sem.at[n], recv_sem=recv_sem.at[kind],
            device_id=(group_at, member_at), device_id_type=MESH,
        )

    def arrive(*rounds):
        rows, kind = 0, None
        for round_of in rounds:
            for n in range(len(SIDES)):
                kind, pairs = round_of(n)
                rows += rows_of(pairs)
        all_of(rows, 0, kind).wait_recv()

    def sent(*rounds):
        for n, (dx, dy) in enumerate(SIDES):
            rows = sum(rows_of(round_of(n)[1]) for round_of in rounds)

            @pl.when(there(dx, dy))
            def _():
                all_of(rows, n, 0).wait_send()

    with phase("start1"):
        share_in_plane()
        share_with_earlier()
        start(first_round)
    with phase("fill"):
        fill_sums()
        for round_of in (first_round, second_coarse, second_fine):
            fill(round_of)

    with phase("w_msum"):
        in_plane.wait_recv()
    part = member_sums[0, row, :]
    for o in range(1, members):
        part = part + member_sums[o, row, :]
    group_sums[0, row, :] = part
    with phase("w_ready"):
        @pl.when(group_at < groups - 1)
        def _():
            pl.semaphore_wait(ready, groups - 1 - group_at)
    share_with_later()
    with phase("w_gsum"):
        from_earlier.wait_recv()
    with phase("w_direct"):
        from_later.wait_recv()
    with phase("mean"):
        total = group_sums[0, row, :]
        later = jnp.zeros((members, cz), f32)
        for o in range(1, groups):
            total = total + group_sums[o, row, :]
            later = later + direct[o]
        total = total + jnp.sum(later, axis=0, keepdims=True)
        mean = jnp.sum(total) / (cx * cy * cz * groups * members)
    with phase("w_halo1"):
        arrive(first_round)

    with phase("masks"):
        edge = lax.broadcasted_iota(jnp.int32, (8, cz), 0) < REACH
        for x in range(3):
            low, own, high = flags[x, 0], flags[x, 1], flags[x, 2]
            low, own, high = (jnp.broadcast_to(v[0:1], (8, cz)) for v in (low, own, high))
            active[x, pl.ds(0, 8), :] = jnp.where(edge, low, own)
            for t in range(1, window // 8 - 1):
                active[x, pl.ds(8 * t, 8), :] = own
            active[x, pl.ds(window - 8, 8), :] = jnp.where(edge, own, high)

    fine_mask = checker(window, cz)

    def half_sweep(t, right, old, other, out, also=None):
        colour = t % 2
        wide_by = (REACH - t + 1) // 2
        rows = pl.ds(ROW0 - REACH, window)
        for region, low, high in ((0, HALO - wide_by, HALO), (1, HALO, HALO + px), (2, HALO + px, HALO + px + wide_by)):
            keep = active[region] > 0.5
            for first in range(low, high, 4):
                planes = range(first, min(first + 4, high))
                sums = neighbours(other, planes, ROW0 - REACH, window, colour, fine_mask, 1)
                for p, nbr in zip(planes, sums):
                    total = right[p, rows, :] - mean + nbr
                    before = old[p, rows, :]
                    out[p, rows, :] = jnp.where(keep, total * SIXTH, before)
                    if also is not None and region == 1:
                        also[p - HALO] = jnp.where(keep, 0.0, total - 6.0 * before)

    with phase("pre"):
        half_sweep(0, mix, mix, black, red)
        half_sweep(1, black_rhs, black, red, mid)
        half_sweep(2, mix, mix, mid, red)
        half_sweep(3, black_rhs, black, red, mid, defect)

    own_mask = checker(cy, cz)

    def red_defects(other, planes):
        sums = neighbours(other, [HALO + a for a in planes], ROW0, cy, 0, own_mask, 1)
        for a, nbr in zip(planes, sums):
            centre = red[HALO + a, own_rows, :]
            yield a, centre, own_rhs[a] - mean + nbr - 6.0 * centre

    with phase("restrict"):
        for first in range(0, px, 4):
            for a, centre, res in red_defects(mid, range(first, first + 4)):
                pair_rows[a] = res + defect[a, pl.ds(REACH, cy), :]
        chosen, even = checker(hy, cz, 2), wide_mask(hy)
        for a in range(hx):
            first, second = (
                pair_rows[2 * a + k, pl.ds(0, hy, stride=2), :] + pair_rows[2 * a + k, pl.ds(1, hy, stride=2), :]
                for k in range(2)
            )
            zero, one = jnp.where(chosen, first, second), jnp.where(chosen, second, first)
            both = jnp.where(even, zero + pltpu.roll(zero, cz - 1, 1), one + pltpu.roll(one, 1, 1))
            mixed[CPLANE0 + a, pl.ds(CROW0, hy), :] = 0.5 * both

    with phase("start2"):
        start(second_coarse)
        start(second_fine)
        for a in range(px):
            own_rhs[a] = own_rhs[a] - mean
    with phase("w_coarse"):
        arrive(second_coarse)

    with phase("coarse"):
        coarse_rows = pl.ds(CROW0 - 8, cwindow)
        coarse_even = wide_mask(cwindow)
        coarse_mask = checker(cwindow, cz, 2)

        def regions(wide_by):
            first, last = CPLANE0, CPLANE0 + hx
            return (0, first - wide_by, first), (1, first, last), (2, last, last + wide_by)

        for region, low, high in regions(COARSE_HALO):
            weight = inside[region]
            for a in range(low, high):
                both = mixed[a, coarse_rows, :]
                s0 = jnp.where(coarse_even, both, pltpu.roll(both, 1, 1))
                rhs0[a, coarse_rows, :] = s0
                rhs1[a, coarse_rows, :] = jnp.where(coarse_even, pltpu.roll(both, cz - 1, 1), both)
                corr0[a, coarse_rows, :] = s0 * weight
        for t in range(1, 2 * COARSE):
            right, other, out = (rhs1, corr0, corr1) if t % 2 else (rhs0, corr1, corr0)
            for region, low, high in regions((COARSE_REACH - t + 1) // 2):
                weight = inside[region]
                for first in range(low, high, 4):
                    planes = range(first, min(first + 4, high))
                    sums = neighbours(other, planes, CROW0 - 8, cwindow, t % 2, coarse_mask, 2)
                    for a, nbr in zip(planes, sums):
                        out[a, coarse_rows, :] = (right[a, coarse_rows, :] + nbr) * weight

    with phase("w_fine2"):
        arrive(second_fine)

    with phase("prolong"):
        half_rows = hy + 8
        rows = pl.ds(CROW0 - 4, half_rows)
        pick = checker(half_rows, cz, 2)
        low_rows, high_rows = pl.ds(ROW0 - 8, 8), pl.ds(ROW0 + cy, 8)
        sub = lax.broadcasted_iota(jnp.int32, (8, cz), 0)
        for p in range(px + 2 * HALO):
            a, k = CPLANE0 + (p - HALO) // 2, (p - HALO) % 2
            c0, c1 = corr0[a, rows, :], corr1[a, rows, :]
            plane = jnp.where(pick, c1, c0) if k else jnp.where(pick, c0, c1)
            wide[p, pl.ds(0, half_rows, stride=2), :] = plane
            wide[p, pl.ds(1, half_rows, stride=2), :] = plane
        for p in range(px + 2 * HALO):
            low, own, high = wide[p, pl.ds(0, 8), :], wide[p, pl.ds(8, cy), :], wide[p, pl.ds(8 + cy, 8), :]
            if HALO <= p < HALO + px:
                post[p, own_rows, :] = mid[p, own_rows, :] + own
                post[p, low_rows, :] = jnp.where(sub == 7, mid[p, low_rows, :], landed[p, low_rows, :]) + low
                post[p, high_rows, :] = jnp.where(sub == 0, mid[p, high_rows, :], landed[p, high_rows, :]) + high
            else:
                post[p, own_rows, :] = landed[p, own_rows, :] + own
                post[p, low_rows, :] = landed[p, low_rows, :] + low
                post[p, high_rows, :] = landed[p, high_rows, :] + high
            if 1 <= p < px + 2 * HALO - 1:
                red[p, own_rows, :] = red[p, own_rows, :] + own
                red[p, low_rows, :] = red[p, low_rows, :] + low
                red[p, high_rows, :] = red[p, high_rows, :] + high

    with phase("post"):
        half_sweep(0, mix, red, post, red)
        half_sweep(1, black_rhs, post, red, post)
        half_sweep(2, mix, red, post, red)
        half_sweep(3, black_rhs, post, red, post, defect)

    with phase("w_sent"):
        sent(first_round, second_coarse, second_fine)
        in_plane.wait_send()
        from_later.wait_send()
        from_earlier.wait_send()


def put(red, post, defect, contrast, smoothed_out, residual_out, smoothed, residual, sem):
    px, cy, cz = contrast.shape
    own_rows = pl.ds(ROW0, cy)
    mask = checker(cy, cz)
    size = px // PIECES
    copies = []
    for piece in range(PIECES):
        planes = range(piece * size, (piece + 1) * size)
        part = pl.ds(2 * piece * size, 2 * size)
        for a in planes:
            centre, value = red[HALO + a, own_rows, :], post[HALO + a, own_rows, :]
            smoothed[2 * a] = jnp.where(mask, centre, value)
            smoothed[2 * a + 1] = jnp.where(mask, value, centre)
        copies.append(pltpu.make_async_copy(smoothed.at[part], smoothed_out.at[part], sem.at[0, piece]))
        copies[-1].start()
        sums = neighbours(post, [HALO + a for a in planes], ROW0, cy, 0, mask, 1)
        for a, nbr in zip(planes, sums):
            res, other = contrast[a] + nbr - 6.0 * red[HALO + a, own_rows, :], defect[a, pl.ds(REACH, cy), :]
            residual[2 * a] = jnp.where(mask, res, other)
            residual[2 * a + 1] = jnp.where(mask, other, res)
        copies.append(pltpu.make_async_copy(residual.at[part], residual_out.at[part], sem.at[1, piece]))
        copies[-1].start()
    for c in copies:
        c.wait()


def per_device(dims, source, potential, refined):
    cx, cy, cz = source.shape
    groups, members = dims
    px, hx, hy = cx // 2, cx // 4, cy // 2
    fine = (px + 2 * HALO, ROW0 + cy + ROW0, cz)
    coarse = (hx + 2 * CPLANE0, hy + 2 * CROW0, cz)
    f32 = jnp.float32
    dma = pltpu.SemaphoreType.DMA
    any_spec = pl.BlockSpec(memory_space=pl.ANY)
    vmem_spec = pl.BlockSpec(memory_space=pltpu.VMEM)
    results = pl.pallas_call(
        functools.partial(kernel, dims, (cx, cy, cz)),
        out_shape=[
            pltpu.VMEM(fine, f32),
            pltpu.VMEM(fine, f32),
            pltpu.VMEM((px, cy + 2 * REACH, cz), f32),
            pltpu.VMEM((px, cy, cz), f32),
        ],
        in_specs=[any_spec] * 3,
        out_specs=[vmem_spec] * 4,
        scratch_shapes=[
            pltpu.SMEM(refined.shape, jnp.int32),
            pltpu.VMEM((2, cx, cy, cz), f32),
            pltpu.VMEM((3, *fine), f32),
            pltpu.VMEM(fine, f32),
            pltpu.VMEM(fine, f32),
            pltpu.VMEM((px, cy, cz), f32),
            pltpu.VMEM(coarse, f32),
            pltpu.VMEM(coarse, f32),
            pltpu.VMEM(coarse, f32),
            pltpu.VMEM(coarse, f32),
            pltpu.VMEM(coarse, f32),
            pltpu.VMEM((px + 2 * HALO, cy + 16, cz), f32),
            pltpu.VMEM((3, 3, 8, cz), f32),
            pltpu.VMEM((3, cy + 2 * REACH, cz), f32),
            pltpu.VMEM((3, hy + 16, cz), f32),
            pltpu.VMEM((members, 8, cz), f32),
            pltpu.VMEM((groups, 8, cz), f32),
            pltpu.VMEM((groups, members, cz), f32),
            pltpu.VMEM((2, px, cy, cz), f32),
            pltpu.VMEM((64 * cy, cz), f32),
            dma((3,)),
            dma((len(SIDES),)),
            dma((3,)),
            dma((6,)),
            pltpu.SemaphoreType.REGULAR,
        ],
        compiler_params=pltpu.CompilerParams(collective_id=0, has_side_effects=True),
    )(refined, source, potential)
    return tuple(pl.pallas_call(
        put,
        out_shape=[jax.ShapeDtypeStruct(source.shape, f32)] * 2,
        in_specs=[vmem_spec] * 4,
        out_specs=[any_spec] * 2,
        scratch_shapes=[pltpu.VMEM(source.shape, f32), pltpu.VMEM(source.shape, f32), dma((2, PIECES))],
    )(*(pltpu.with_memory_space_constraint(v, pltpu.VMEM) for v in results)))


def solution(mesh):
    spec = P("group", "member", None)
    return jax.shard_map(
        functools.partial(per_device, (mesh.shape["group"], mesh.shape["member"])),
        mesh=mesh,
        in_specs=(spec, spec, spec),
        out_specs=(spec, spec),
        check_vma=False,
    )
```

```python
import contextlib
import functools

import jax
import jax.numpy as jnp
from jax import lax
from jax.experimental import pallas as pl
from jax.experimental.pallas import tpu as pltpu
from jax.sharding import PartitionSpec as P

SWEEPS = 2
COARSE = 2
REACH = 2 * SWEEPS
HALO = (REACH + 2) // 2
COARSE_REACH = 2 * COARSE - 1 + (REACH + 2) // 2
COARSE_HALO = COARSE_REACH // 2
ROW0 = 8 + REACH
CROW0 = 16
CPLANE0 = COARSE_HALO + 1
SIDES = ((0, -1), (0, 1), (-1, 0), (1, 0), (-1, -1), (-1, 1), (1, -1), (1, 1))
MESH = pl.DeviceIdType.MESH
SIXTH = 1.0 / 6.0
DETOUR = 2
PIECES = 4


def phase(name):
    return contextlib.nullcontext()


def span(side, begin, end, first, count):
    if side == 0:
        return pl.ds(first, count), pl.ds(first, count)
    if side > 0:
        return pl.ds(first + count - end, end - begin), pl.ds(first - end, end - begin)
    return pl.ds(first + begin, end - begin), pl.ds(first + count + begin, end - begin)


def checker(rows, cz, lanes_per=1):
    r = lax.broadcasted_iota(jnp.int32, (rows, cz), 0)
    return ((r + lax.broadcasted_iota(jnp.int32, (rows, cz), 1) // lanes_per) & 1) == 0


def lanes(value, step):
    cz = value.shape[1]
    lane = lax.broadcasted_iota(jnp.int32, value.shape, 1)
    low = jnp.where(lane < step, 0.0, pltpu.roll(value, step, 1))
    high = jnp.where(lane >= cz - step, 0.0, pltpu.roll(value, cz - step, 1))
    return low + high


def neighbours(other, planes, row, rows, colour, mask, step):
    centres = {}
    out = []
    for p in planes:
        for q in (p - 1, p, p + 1):
            if q not in centres:
                centres[q] = other[q, pl.ds(row, rows), :]
        near, far = (centres[p - 1], centres[p + 1]) if colour == 0 else (centres[p + 1], centres[p - 1])
        total = centres[p] + jnp.where(mask, near, far)
        total = total + (other[p, pl.ds(row - 1, rows), :] + other[p, pl.ds(row + 1, rows), :])
        out.append(total + lanes(centres[p], step))
    return out


def kernel(
    dims, sizes,
    refined_hbm, source_ref, potential_ref,
    red, post, defect, own_rhs,
    refined_ref, raw, field, mid, landed, pair_rows, mixed, rhs0, rhs1, corr0, corr1, wide,
    flags, active, inside, member_sums, group_sums, direct, passing, unit_red, unit_black, zeros, dummy,
    local_sem, send_sem, recv_sem, sum_sem, pass_sem, ready,
):
    groups, members = dims
    cx, cy, cz = sizes
    px, hx, hy = cx // 2, cx // 4, cy // 2
    group_at = lax.axis_index("group")
    member_at = lax.axis_index("member")
    f32 = jnp.float32
    black, mix, black_rhs = field.at[0], field.at[1], field.at[2]
    own_rows = pl.ds(ROW0, cy)
    window = cy + 2 * REACH
    cwindow = hy + 16

    load_source = pltpu.make_async_copy(source_ref, raw.at[0], local_sem.at[0])
    load_potential = pltpu.make_async_copy(potential_ref, raw.at[1], local_sem.at[1])
    load_refined = pltpu.make_async_copy(refined_hbm, refined_ref, local_sem.at[2])
    load_source.start()
    load_potential.start()
    load_refined.start()

    def there(dx, dy):
        ok = None
        for side, at, count in ((dx, group_at, groups), (dy, member_at, members)):
            if side == 0:
                continue
            here = at > 0 if side < 0 else at < count - 1
            ok = here if ok is None else ok & here
        return ok

    def device(dx, dy):
        return (group_at + dx, member_at + dy)

    def signal(sem, at):
        pl.semaphore_signal(sem, inc=1, device_id=at, device_id_type=MESH)

    barrier = pltpu.get_barrier_semaphore()
    for o in range(1, members):
        signal(barrier, (group_at, lax.rem(member_at + o, members)))
    expected = jnp.int32(members - 1) + group_at * members
    for dy in (-1, 0, 1):
        @pl.when(there(-1, dy))
        def _():
            signal(barrier, device(-1, dy))
        expected = expected + there(1, dy).astype(jnp.int32)

    def greet(o, carry):
        for m in range(members):
            signal(barrier, (group_at + o, m))
        return carry

    lax.fori_loop(1, groups - group_at, greet, 0)

    blank_rows = jnp.zeros((cy, cz), f32)
    for kind in range(2):
        for p in range(px):
            zeros[kind, p] = blank_rows
    blank_coarse = jnp.zeros((cwindow, cz), f32)
    for a in range(hx + 2 * CPLANE0):
        mixed[a, pl.ds(CROW0 - 8, cwindow), :] = blank_coarse
    for a in (0, hx + 2 * CPLANE0 - 1):
        corr0[a, pl.ds(CROW0 - 8, cwindow), :] = blank_coarse

    crow = lax.broadcasted_iota(jnp.int32, (cwindow, cz), 0) - 8
    clow = jnp.where(member_at > 0, -8, 0)
    chigh = jnp.where(member_at < members - 1, hy + 8, hy)
    within = jnp.where((crow >= clow) & (crow < chigh), SIXTH, 0.0)
    for region in range(3):
        alive = 1.0 if region == 1 else there(region - 1, 0).astype(f32)
        inside[region] = within * alive

    def wide_mask(rows):
        return lax.broadcasted_iota(jnp.int32, (rows, cz), 1) % 2 == 0

    with phase("load"):
        load_refined.wait()
        lane1 = lax.broadcasted_iota(jnp.int32, (1, cz), 1)
        boxes = refined_ref.shape[2]
        box = cz // boxes
        marks = jnp.zeros((1, cz), jnp.int32)
        for b in range(boxes):
            marks = jnp.where(lane1 // box == b, jnp.full((1, cz), refined_ref[0, 0, b], jnp.int32), marks)
        flags[1, 1, pl.ds(0, 1), :] = (marks == 1).astype(f32)
        load_source.wait()
        load_potential.wait()

    with phase("pack"):
        here = checker(cy, cz)
        smooth_own = jnp.broadcast_to(flags[1, 1, 0:1, :], (cy, cz)) > 0.5
        acc = [jnp.zeros((8, cz), f32)] * 4
        for a in range(px):
            s0, s1 = raw[0, 2 * a], raw[0, 2 * a + 1]
            v0, v1 = raw[1, 2 * a], raw[1, 2 * a + 1]
            both = s0 + s1
            acc = [acc[t] + sum(both[8 * u:8 * u + 8] for u in range(t, cy // 8, 4)) for t in range(4)]
            red_rhs = jnp.where(here, s0, s1)
            own_rhs[a] = red_rhs
            mix[HALO + a, own_rows, :] = jnp.where(smooth_own, red_rhs, jnp.where(here, v0, v1))
            black[HALO + a, own_rows, :] = jnp.where(here, v1, v0)
            black_rhs[HALO + a, own_rows, :] = jnp.where(here, s1, s0)
        acc = (acc[0] + acc[1]) + (acc[2] + acc[3])
        member_sums[0, pl.ds(0, 1), :] = jnp.sum(acc, axis=0, keepdims=True)

    with phase("barrier"):
        pl.semaphore_wait(barrier, expected)

    def report(g, carry):
        signal(ready, (g, member_at))
        return carry

    lax.fori_loop(0, group_at, report, 0)

    row = pl.ds(0, 1)

    def sum_copy(src, dst, n, at):
        return pltpu.make_async_remote_copy(
            src_ref=src, dst_ref=dst, send_sem=sum_sem.at[n], recv_sem=sum_sem.at[n + 1], device_id=at, device_id_type=MESH,
        )

    own_sum, plane_sum = member_sums.at[0, row], group_sums.at[0, row]
    no_sum = zeros.at[0, 0, row]

    def share_in_plane():
        for o in range(1, members):
            sum_copy(own_sum, member_sums.at[o, row], 0, (group_at, lax.rem(member_at + o, members))).start()

    def share_with_earlier():
        for o in range(groups - 1, 0, -1):
            @pl.when(group_at >= o)
            def _():
                for m in range(members):
                    sum_copy(own_sum, direct.at[o, pl.ds(member_at, 1)], 2, (group_at - o, m)).start()

    def fill_sums():
        for o in range(1, groups):
            @pl.when(group_at < o)
            def _():
                pltpu.make_async_copy(zeros.at[0, 0, pl.ds(0, members)], dummy.at[pl.ds(o * members, members)], sum_sem.at[2]).start()
                pltpu.make_async_copy(no_sum, group_sums.at[o, row], sum_sem.at[5]).start()

            @pl.when(group_at + o >= groups)
            def _():
                pltpu.make_async_copy(zeros.at[0, 0, pl.ds(0, members)], direct.at[o], sum_sem.at[3]).start()
                pltpu.make_async_copy(no_sum, dummy.at[pl.ds(groups * members + o, 1)], sum_sem.at[4]).start()

    def share_with_later():
        for o in range(1, groups):
            @pl.when(group_at + o < groups)
            def _():
                sum_copy(plane_sum, group_sums.at[o, row], 4, (group_at + o, member_at)).start()

    def sums(slots, n):
        return sum_copy(slots, slots, n, (group_at, member_at))

    in_plane = sums(member_sums.at[pl.ds(1, members - 1), row], 0)
    from_later = sums(direct.at[pl.ds(1, groups - 1)], 2)
    from_earlier = sums(group_sums.at[pl.ds(1, groups - 1), row], 4)

    def marks_round(n):
        dx, dy = SIDES[n]
        return 4, [(flags.at[1, 1, row], flags.at[1 - dx, 1 - dy, row])]

    def first_round(n):
        dx, dy = SIDES[n]
        pairs = []
        if dx and dy:
            pieces = ((0, 1, 0, 1, 4), (1, 1, 0, 1, 3), (2, 1, 0, 1, 2), (0, 1, 1, 2, 2), (1, 1, 1, 2, 1))
        elif dx:
            pieces = ((0, 1, 0, HALO, cy), (1, 2, 0, HALO - 1, cy))
        else:
            pieces = ((0, 1, 0, px, REACH + 1), (1, 1, 0, px, REACH), (2, 1, 0, px, REACH - 1))
        for kind, kinds, begin, end, deep in pieces:
            sx, tx = span(dx, begin, end, HALO, px)
            sy, ty = span(dy, 0, deep, ROW0, cy)
            pairs.append((field.at[pl.ds(kind, kinds), sx, sy], field.at[pl.ds(kind, kinds), tx, ty]))
        return (3 if dy else 0), pairs

    def second_coarse(n):
        dx, dy = SIDES[n]
        if dx and dy:
            pieces = ((0, 1, 5), (1, 2, 3), (2, 3, 1))
        elif dx:
            pieces = ((0, COARSE_HALO, hy),)
        else:
            pieces = ((0, hx, COARSE_REACH),)
        pairs = []
        for begin, end, deep in pieces:
            sx, tx = span(dx, begin, end, CPLANE0, hx)
            sy, ty = span(dy, 0, deep, CROW0, hy)
            pairs.append((mixed.at[sx, sy], mixed.at[tx, ty]))
        return 1, pairs

    def second_fine(n):
        dx, dy = SIDES[n]
        if dx and dy:
            pieces = ((0, 1, 0, 4), (1, 2, 0, 2))
        elif dx:
            pieces = ((0, HALO, 0, cy),)
        else:
            pieces = ((0, px, 1, REACH + 1),)
        pairs = []
        for begin, end, skip, deep in pieces:
            sx, tx = span(dx, begin, end, HALO, px)
            sy, ty = span(dy, skip, deep, ROW0, cy)
            pairs.append((mid.at[sx, sy], landed.at[tx, ty]))
        return 2, pairs

    def rows_of(pairs):
        total = 0
        for _, dst in pairs:
            total += functools.reduce(lambda p, q: p * q, dst.shape[:-1])
        return total

    odd = lax.rem(member_at, 2) == 1

    def start(round_of):
        for far in (True, None, False):
            for n, (dx, dy) in enumerate(SIDES):
                if (dy == 0) != (far is None):
                    continue
                kind, pairs = round_of(n)
                now = there(dx, dy)
                if far is not None:
                    now = now & (odd if (dy > 0) == far else jnp.logical_not(odd))

                @pl.when(now)
                def _():
                    split = via and far and not dx and round_of is first_round
                    if split:
                        send_face(n)
                    for src, dst in () if split else pairs:
                        pltpu.make_async_remote_copy(
                            src_ref=src, dst_ref=dst, send_sem=send_sem.at[n], recv_sem=recv_sem.at[kind],
                            device_id=device(dx, dy), device_id_type=MESH,
                        ).start()

    around = px * DETOUR // 8
    via = members % 2 == 0
    detour = []
    at_row = 0
    for kind, deep in ((0, REACH + 1), (1, REACH), (2, REACH - 1)):
        detour.append((kind, deep, pl.ds(at_row, deep)))
        at_row += deep
    detour_rows = at_row * around
    direct_planes, around_planes = pl.ds(HALO, px - around), pl.ds(HALO + px - around, around)

    def send_face(n):
        dx, dy = SIDES[n]
        for by_detour in (True, False):
            for kind, deep, rows in detour:
                sy, ty = span(dy, 0, deep, ROW0, cy)
                planes = around_planes if by_detour else direct_planes
                pltpu.make_async_remote_copy(
                    src_ref=field.at[kind, planes, sy],
                    dst_ref=passing.at[pl.ds(0, around), rows] if by_detour else field.at[kind, planes, ty],
                    send_sem=send_sem.at[n], recv_sem=pass_sem.at[0] if by_detour else recv_sem.at[3],
                    device_id=device(0, 2 * dy if by_detour else dy), device_id_type=MESH,
                ).start()

    def passes(side):
        return (odd & (member_at >= 2)) if side < 0 else (jnp.logical_not(odd) & (member_at + 2 < members))

    def passed():
        part = dummy.at[pl.ds(0, detour_rows)]
        return pltpu.make_async_remote_copy(
            src_ref=part, dst_ref=part, send_sem=pass_sem.at[1], recv_sem=pass_sem.at[0],
            device_id=(group_at, member_at), device_id_type=MESH,
        )

    def pass_on(now):
        for side in (-1, 1):
            @pl.when(passes(side) & now)
            def _():
                passed().wait_recv()
                for kind, deep, rows in detour:
                    ty = span(-side, 0, deep, ROW0, cy)[1]
                    pltpu.make_async_remote_copy(
                        src_ref=passing.at[pl.ds(0, around), rows], dst_ref=field.at[kind, around_planes, ty],
                        send_sem=pass_sem.at[1], recv_sem=recv_sem.at[3],
                        device_id=device(0, side), device_id_type=MESH,
                    ).start()

    def fill(round_of):
        for n, (dx, dy) in enumerate(SIDES):
            kind, pairs = round_of(n)
            @pl.when(jnp.logical_not(there(-dx, -dy)))
            def _():
                for _, dst in pairs:
                    shape = dst.shape[:-1]
                    src = zeros.at[(0,) * (4 - len(dst.shape)) + tuple(pl.ds(0, size) for size in shape)]
                    pltpu.make_async_copy(src, dst, recv_sem.at[kind]).start()

    def all_of(rows, n, kind):
        part = dummy.at[pl.ds(0, rows)]
        return pltpu.make_async_remote_copy(
            src_ref=part, dst_ref=part, send_sem=send_sem.at[n], recv_sem=recv_sem.at[kind],
            device_id=(group_at, member_at), device_id_type=MESH,
        )

    def arrive(round_of, kind):
        arriving = (round_of(n) for n in range(len(SIDES)))
        all_of(sum(rows_of(pairs) for which, pairs in arriving if which == kind), 0, kind).wait_recv()

    def sent(*rounds):
        for n, (dx, dy) in enumerate(SIDES):
            rows = sum(rows_of(round_of(n)[1]) for round_of in rounds)

            @pl.when(there(dx, dy))
            def _():
                all_of(rows, n, 0).wait_send()

    with phase("start1"):
        share_in_plane()
        share_with_earlier()
        start(marks_round)
        start(first_round)
    with phase("fill"):
        fill_sums()
        for round_of in (marks_round, first_round, second_coarse, second_fine):
            fill(round_of)

    with phase("w_msum"):
        in_plane.wait_recv()
    part = member_sums[0, row, :]
    for o in range(1, members):
        part = part + member_sums[o, row, :]
    group_sums[0, row, :] = part
    if via:
        with phase("pass1"):
            pass_on(group_at < 2)
    with phase("w_ready"):
        @pl.when(group_at < groups - 1)
        def _():
            pl.semaphore_wait(ready, groups - 1 - group_at)
    share_with_later()
    if via:
        with phase("pass2"):
            pass_on(group_at >= 2)
    def plane_groups(t):
        wide_by = (REACH - t + 1) // 2
        for region, low, high in ((0, HALO - wide_by, HALO), (1, HALO, HALO + px), (2, HALO + px, HALO + px + wide_by)):
            for first in range(low, high, 4):
                yield region, range(first, min(first + 4, high))

    fine_mask = checker(window, cz)
    stages = ((mix, mix, black, red), (black_rhs, black, red, mid), (mix, red, mid, red), (black_rhs, mid, red, mid))

    with phase("w_marks"):
        arrive(marks_round, 4)
    with phase("masks"):
        edge = lax.broadcasted_iota(jnp.int32, (8, cz), 0) < REACH
        for x in range(3):
            low, own, high = flags[x, 0], flags[x, 1], flags[x, 2]
            low, own, high = (jnp.broadcast_to(v[0:1], (8, cz)) for v in (low, own, high))
            active[x, pl.ds(0, 8), :] = jnp.where(edge, low, own)
            for t in range(1, window // 8 - 1):
                active[x, pl.ds(8 * t, 8), :] = own
            active[x, pl.ds(window - 8, 8), :] = jnp.where(edge, own, high)

    with phase("unit"):
        rows = pl.ds(ROW0 - REACH, window)
        for p in range(HALO - 2, HALO + px + 2):
            region = 0 if p < HALO else 1 if p < HALO + px else 2
            unit_red[p, rows, :] = active[region] * SIXTH
        for t, other, out in ((1, unit_red, unit_black), (2, unit_black, unit_red)):
            for region, planes in plane_groups(t):
                weight = active[region] * SIXTH
                sums = neighbours(other, planes, ROW0 - REACH, window, t % 2, fine_mask, 1)
                for p, nbr in zip(planes, sums):
                    out[p, rows, :] = (1.0 + nbr) * weight

    with phase("w_along"):
        arrive(first_round, 0)
    with phase("inner"):
        inner = cy - 2
        inner_rows = pl.ds(ROW0 + 1, inner)
        at = lax.broadcasted_iota(jnp.int32, (inner, cz), 0)
        inner_mask = jnp.logical_not(checker(inner, cz))
        smoothed = [jnp.broadcast_to(flags[x, 1, row, :], (inner, cz)) > 0.5 for x in range(3)]
        for t, (right, old, other, out) in enumerate(stages[:-1]):
            reached = (at >= t) & (at < inner - t)
            for region, planes in plane_groups(t):
                keep = smoothed[region] & reached
                sums = neighbours(other, planes, ROW0 + 1, inner, t % 2, inner_mask, 1)
                for p, nbr in zip(planes, sums):
                    total = right[p, inner_rows, :] + nbr
                    out[p, inner_rows, :] = jnp.where(keep, total * SIXTH, old[p, inner_rows, :])

    with phase("w_halo1"):
        arrive(first_round, 3)

    with phase("edges"):
        edge_mask = checker(8, cz)
        sub = lax.broadcasted_iota(jnp.int32, (8, cz), 0)
        for t, (right, old, other, out) in enumerate(stages[:-1]):
            for region, planes in plane_groups(t):
                for low in (True, False):
                    first = ROW0 - REACH if low else ROW0 + cy - REACH
                    rows = pl.ds(first, 8)
                    keep = active[region, pl.ds(first - ROW0 + REACH, 8), :] > 0.5
                    fresh = (sub <= REACH + t) if low else (sub >= REACH - 1 - t)
                    sums = neighbours(other, planes, first, 8, t % 2, edge_mask, 1)
                    for p, nbr in zip(planes, sums):
                        total = right[p, rows, :] + nbr
                        value = jnp.where(keep, total * SIXTH, old[p, rows, :])
                        out[p, rows, :] = jnp.where(fresh, value, out[p, rows, :])

    with phase("w_gsum"):
        from_earlier.wait_recv()
    with phase("w_direct"):
        from_later.wait_recv()
    with phase("mean"):
        total = group_sums[0, row, :]
        later = jnp.zeros((members, cz), f32)
        for o in range(1, groups):
            total = total + group_sums[o, row, :]
            later = later + direct[o]
        total = total + jnp.sum(later, axis=0, keepdims=True)
        mean = jnp.sum(total) / (cx * cy * cz * groups * members)

    def black_sweep(right, other, out):
        rows = pl.ds(ROW0 - REACH, window)
        for region, planes in plane_groups(REACH - 1):
            keep = active[region] > 0.5
            sums = neighbours(other, planes, ROW0 - REACH, window, 1, fine_mask, 1)
            for p, nbr in zip(planes, sums):
                total = right[p, rows, :] - mean + nbr
                before = out[p, rows, :]
                out[p, rows, :] = jnp.where(keep, total * SIXTH, before)
                if region == 1:
                    defect[p - HALO] = jnp.where(keep, 0.0, total - 6.0 * before)

    with phase("last_pre"):
        rows = pl.ds(ROW0 - REACH, window)
        for p in range(HALO - 1, HALO + px + 1):
            red[p, rows, :] = red[p, rows, :] - mean * unit_red[p, rows, :]
        black_sweep(black_rhs, red, mid)

    own_mask = checker(cy, cz)

    def red_defects(other, planes):
        sums = neighbours(other, [HALO + a for a in planes], ROW0, cy, 0, own_mask, 1)
        for a, nbr in zip(planes, sums):
            centre = red[HALO + a, own_rows, :]
            yield a, centre, own_rhs[a] - mean + nbr - 6.0 * centre

    with phase("restrict"):
        for first in range(0, px, 4):
            for a, centre, res in red_defects(mid, range(first, first + 4)):
                pair_rows[a] = res + defect[a, pl.ds(REACH, cy), :]
        chosen, even = checker(hy, cz, 2), wide_mask(hy)
        for a in range(hx):
            first, second = (
                pair_rows[2 * a + k, pl.ds(0, hy, stride=2), :] + pair_rows[2 * a + k, pl.ds(1, hy, stride=2), :]
                for k in range(2)
            )
            zero, one = jnp.where(chosen, first, second), jnp.where(chosen, second, first)
            both = jnp.where(even, zero + pltpu.roll(zero, cz - 1, 1), one + pltpu.roll(one, 1, 1))
            mixed[CPLANE0 + a, pl.ds(CROW0, hy), :] = 0.5 * both

    with phase("start2"):
        start(second_coarse)
        start(second_fine)
        for a in range(px):
            own_rhs[a] = own_rhs[a] - mean
    with phase("w_coarse"):
        arrive(second_coarse, 1)

    with phase("coarse"):
        coarse_rows = pl.ds(CROW0 - 8, cwindow)
        coarse_even = wide_mask(cwindow)
        coarse_mask = checker(cwindow, cz, 2)

        def regions(wide_by):
            first, last = CPLANE0, CPLANE0 + hx
            return (0, first - wide_by, first), (1, first, last), (2, last, last + wide_by)

        for region, low, high in regions(COARSE_HALO):
            weight = inside[region]
            for a in range(low, high):
                both = mixed[a, coarse_rows, :]
                s0 = jnp.where(coarse_even, both, pltpu.roll(both, 1, 1))
                rhs0[a, coarse_rows, :] = s0
                rhs1[a, coarse_rows, :] = jnp.where(coarse_even, pltpu.roll(both, cz - 1, 1), both)
                corr0[a, coarse_rows, :] = s0 * weight
        for t in range(1, 2 * COARSE):
            right, other, out = (rhs1, corr0, corr1) if t % 2 else (rhs0, corr1, corr0)
            for region, low, high in regions((COARSE_REACH - t + 1) // 2):
                weight = inside[region]
                for first in range(low, high, 4):
                    planes = range(first, min(first + 4, high))
                    sums = neighbours(other, planes, CROW0 - 8, cwindow, t % 2, coarse_mask, 2)
                    for a, nbr in zip(planes, sums):
                        out[a, coarse_rows, :] = (right[a, coarse_rows, :] + nbr) * weight

    with phase("w_fine2"):
        arrive(second_fine, 2)

    with phase("prolong"):
        half_rows = hy + 8
        rows = pl.ds(CROW0 - 4, half_rows)
        pick = checker(half_rows, cz, 2)
        low_rows, high_rows = pl.ds(ROW0 - 8, 8), pl.ds(ROW0 + cy, 8)
        sub = lax.broadcasted_iota(jnp.int32, (8, cz), 0)
        for p in range(px + 2 * HALO):
            a, k = CPLANE0 + (p - HALO) // 2, (p - HALO) % 2
            c0, c1 = corr0[a, rows, :], corr1[a, rows, :]
            plane = jnp.where(pick, c1, c0) if k else jnp.where(pick, c0, c1)
            wide[p, pl.ds(0, half_rows, stride=2), :] = plane
            wide[p, pl.ds(1, half_rows, stride=2), :] = plane
        for p in range(px + 2 * HALO):
            low, own, high = wide[p, pl.ds(0, 8), :], wide[p, pl.ds(8, cy), :], wide[p, pl.ds(8 + cy, 8), :]
            if HALO <= p < HALO + px:
                post[p, own_rows, :] = mid[p, own_rows, :] + own
                post[p, low_rows, :] = jnp.where(sub == 7, mid[p, low_rows, :], landed[p, low_rows, :]) + low
                post[p, high_rows, :] = jnp.where(sub == 0, mid[p, high_rows, :], landed[p, high_rows, :]) + high
            else:
                post[p, own_rows, :] = landed[p, own_rows, :] + own
                post[p, low_rows, :] = landed[p, low_rows, :] + low
                post[p, high_rows, :] = landed[p, high_rows, :] + high
            if 1 <= p < px + 2 * HALO - 1:
                red[p, own_rows, :] = red[p, own_rows, :] + own
                red[p, low_rows, :] = red[p, low_rows, :] + low
                red[p, high_rows, :] = red[p, high_rows, :] + high

    with phase("post"):
        rows = pl.ds(ROW0 - REACH, window)
        for t in range(REACH - 1):
            right, other, out = (black_rhs, red, post) if t % 2 else (mix, post, red)
            for region, planes in plane_groups(t):
                keep = active[region] > 0.5
                sums = neighbours(other, planes, ROW0 - REACH, window, t % 2, fine_mask, 1)
                for p, nbr in zip(planes, sums):
                    total = right[p, rows, :] - mean + nbr
                    out[p, rows, :] = jnp.where(keep, total * SIXTH, out[p, rows, :])
        black_sweep(black_rhs, red, post)

    with phase("w_sent"):
        sent(marks_round, first_round, second_coarse, second_fine)
        if via:
            for side in (-1, 1):
                @pl.when(passes(side))
                def _():
                    passed().wait_send()
        in_plane.wait_send()
        from_later.wait_send()
        from_earlier.wait_send()


def put(red, post, defect, contrast, smoothed_out, residual_out, smoothed, residual, sem):
    px, cy, cz = contrast.shape
    own_rows = pl.ds(ROW0, cy)
    mask = checker(cy, cz)
    copies = []

    def send(n, src, dst, first, size):
        part = pl.ds(2 * first, 2 * size)
        copies.append(pltpu.make_async_copy(src.at[part], dst.at[part], sem.at[n]))
        copies[-1].start()

    for a in range(px):
        centre, value = red[HALO + a, own_rows, :], post[HALO + a, own_rows, :]
        smoothed[2 * a] = jnp.where(mask, centre, value)
        smoothed[2 * a + 1] = jnp.where(mask, value, centre)
    send(0, smoothed, smoothed_out, 0, px)
    size = px // PIECES
    for piece in range(PIECES):
        planes = range(piece * size, (piece + 1) * size)
        sums = neighbours(post, [HALO + a for a in planes], ROW0, cy, 0, mask, 1)
        for a, nbr in zip(planes, sums):
            res, other = contrast[a] + nbr - 6.0 * red[HALO + a, own_rows, :], defect[a, pl.ds(REACH, cy), :]
            residual[2 * a] = jnp.where(mask, res, other)
            residual[2 * a + 1] = jnp.where(mask, other, res)
        send(1 + piece, residual, residual_out, piece * size, size)
    for c in copies:
        c.wait()


def per_device(dims, source, potential, refined):
    cx, cy, cz = source.shape
    groups, members = dims
    px, hx, hy = cx // 2, cx // 4, cy // 2
    fine = (px + 2 * HALO, ROW0 + cy + ROW0, cz)
    coarse = (hx + 2 * CPLANE0, hy + 2 * CROW0, cz)
    f32 = jnp.float32
    dma = pltpu.SemaphoreType.DMA
    any_spec = pl.BlockSpec(memory_space=pl.ANY)
    vmem_spec = pl.BlockSpec(memory_space=pltpu.VMEM)
    results = pl.pallas_call(
        functools.partial(kernel, dims, (cx, cy, cz)),
        out_shape=[
            pltpu.VMEM(fine, f32),
            pltpu.VMEM(fine, f32),
            pltpu.VMEM((px, cy + 2 * REACH, cz), f32),
            pltpu.VMEM((px, cy, cz), f32),
        ],
        in_specs=[any_spec] * 3,
        out_specs=[vmem_spec] * 4,
        scratch_shapes=[
            pltpu.SMEM(refined.shape, jnp.int32),
            pltpu.VMEM((2, cx, cy, cz), f32),
            pltpu.VMEM((3, *fine), f32),
            pltpu.VMEM(fine, f32),
            pltpu.VMEM(fine, f32),
            pltpu.VMEM((px, cy, cz), f32),
            pltpu.VMEM(coarse, f32),
            pltpu.VMEM(coarse, f32),
            pltpu.VMEM(coarse, f32),
            pltpu.VMEM(coarse, f32),
            pltpu.VMEM(coarse, f32),
            pltpu.VMEM((px + 2 * HALO, cy + 16, cz), f32),
            pltpu.VMEM((3, 3, 8, cz), f32),
            pltpu.VMEM((3, cy + 2 * REACH, cz), f32),
            pltpu.VMEM((3, hy + 16, cz), f32),
            pltpu.VMEM((members, 8, cz), f32),
            pltpu.VMEM((groups, 8, cz), f32),
            pltpu.VMEM((groups, members, cz), f32),
            pltpu.VMEM((px, 16, cz), f32),
            pltpu.VMEM(fine, f32),
            pltpu.VMEM(fine, f32),
            pltpu.VMEM((2, px, cy, cz), f32),
            pltpu.VMEM((64 * cy, cz), f32),
            dma((3,)),
            dma((len(SIDES),)),
            dma((5,)),
            dma((6,)),
            dma((2,)),
            pltpu.SemaphoreType.REGULAR,
        ],
        compiler_params=pltpu.CompilerParams(collective_id=0, has_side_effects=True),
    )(refined, source, potential)
    return tuple(pl.pallas_call(
        put,
        out_shape=[jax.ShapeDtypeStruct(source.shape, f32)] * 2,
        in_specs=[vmem_spec] * 4,
        out_specs=[any_spec] * 2,
        scratch_shapes=[pltpu.VMEM(source.shape, f32), pltpu.VMEM(source.shape, f32), dma((1 + PIECES,))],
    )(*(pltpu.with_memory_space_constraint(v, pltpu.VMEM) for v in results)))


def solution(mesh):
    spec = P("group", "member", None)
    return jax.shard_map(
        functools.partial(per_device, (mesh.shape["group"], mesh.shape["member"])),
        mesh=mesh,
        in_specs=(spec, spec, spec),
        out_specs=(spec, spec),
        check_vma=False,
    )
```

```python
import contextlib
import functools

import jax
import jax.numpy as jnp
from jax import lax
from jax.experimental import pallas as pl
from jax.experimental.pallas import tpu as pltpu
from jax.sharding import PartitionSpec as P

SWEEPS = 2
COARSE = 2
REACH = 2 * SWEEPS
HALO = (REACH + 2) // 2
COARSE_REACH = 2 * COARSE - 1 + (REACH + 2) // 2
COARSE_HALO = COARSE_REACH // 2
ROW0 = 8 + REACH
CROW0 = 16
CPLANE0 = COARSE_HALO + 1
SIDES = ((0, -1), (0, 1), (-1, 0), (1, 0), (-1, -1), (-1, 1), (1, -1), (1, 1))
MESH = pl.DeviceIdType.MESH
SIXTH = 1.0 / 6.0
DETOUR = 2
PIECES = 4


def phase(name):
    return contextlib.nullcontext()


def span(side, begin, end, first, count):
    if side == 0:
        return pl.ds(first, count), pl.ds(first, count)
    if side > 0:
        return pl.ds(first + count - end, end - begin), pl.ds(first - end, end - begin)
    return pl.ds(first + begin, end - begin), pl.ds(first + count + begin, end - begin)


def checker(rows, cz, lanes_per=1):
    r = lax.broadcasted_iota(jnp.int32, (rows, cz), 0)
    return ((r + lax.broadcasted_iota(jnp.int32, (rows, cz), 1) // lanes_per) & 1) == 0


def lanes(value, step):
    cz = value.shape[1]
    lane = lax.broadcasted_iota(jnp.int32, value.shape, 1)
    low = jnp.where(lane < step, 0.0, pltpu.roll(value, step, 1))
    high = jnp.where(lane >= cz - step, 0.0, pltpu.roll(value, cz - step, 1))
    return low + high


def neighbours(other, planes, row, rows, colour, mask, step):
    centres = {}
    out = []
    for p in planes:
        for q in (p - 1, p, p + 1):
            if q not in centres:
                centres[q] = other[q, pl.ds(row, rows), :]
        near, far = (centres[p - 1], centres[p + 1]) if colour == 0 else (centres[p + 1], centres[p - 1])
        total = centres[p] + jnp.where(mask, near, far)
        total = total + (other[p, pl.ds(row - 1, rows), :] + other[p, pl.ds(row + 1, rows), :])
        out.append(total + lanes(centres[p], step))
    return out


def kernel(
    dims, sizes,
    refined_hbm, source_ref, potential_ref,
    red, post, defect, own_rhs,
    refined_ref, raw, field, mid, landed, pair_rows, mixed, rhs0, rhs1, corr0, corr1, wide,
    flags, active, inside, member_sums, group_sums, direct, passing, unit_red, unit_black, zeros, dummy,
    local_sem, send_sem, recv_sem, sum_sem, pass_sem, ready,
):
    groups, members = dims
    cx, cy, cz = sizes
    px, hx, hy = cx // 2, cx // 4, cy // 2
    group_at = lax.axis_index("group")
    member_at = lax.axis_index("member")
    f32 = jnp.float32
    black, mix, black_rhs = field.at[0], field.at[1], field.at[2]
    own_rows = pl.ds(ROW0, cy)
    window = cy + 2 * REACH
    cwindow = hy + 16

    load_source = pltpu.make_async_copy(source_ref, raw.at[0], local_sem.at[0])
    load_potential = pltpu.make_async_copy(potential_ref, raw.at[1], local_sem.at[1])
    load_refined = pltpu.make_async_copy(refined_hbm, refined_ref, local_sem.at[2])
    load_source.start()
    load_potential.start()
    load_refined.start()

    def there(dx, dy):
        ok = None
        for side, at, count in ((dx, group_at, groups), (dy, member_at, members)):
            if side == 0:
                continue
            here = at > 0 if side < 0 else at < count - 1
            ok = here if ok is None else ok & here
        return ok

    def device(dx, dy):
        return (group_at + dx, member_at + dy)

    def signal(sem, at):
        pl.semaphore_signal(sem, inc=1, device_id=at, device_id_type=MESH)

    barrier = pltpu.get_barrier_semaphore()
    for o in range(1, members):
        signal(barrier, (group_at, lax.rem(member_at + o, members)))
    expected = jnp.int32(members - 1) + group_at * members
    for dy in (-1, 0, 1):
        @pl.when(there(-1, dy))
        def _():
            signal(barrier, device(-1, dy))
        expected = expected + there(1, dy).astype(jnp.int32)

    def greet(o, carry):
        for m in range(members):
            signal(barrier, (group_at + o, m))
        return carry

    lax.fori_loop(1, groups - group_at, greet, 0)

    blank_rows = jnp.zeros((cy, cz), f32)
    for kind in range(2):
        for p in range(px):
            zeros[kind, p] = blank_rows
    blank_coarse = jnp.zeros((cwindow, cz), f32)
    for a in range(hx + 2 * CPLANE0):
        mixed[a, pl.ds(CROW0 - 8, cwindow), :] = blank_coarse
    for a in (0, hx + 2 * CPLANE0 - 1):
        corr0[a, pl.ds(CROW0 - 8, cwindow), :] = blank_coarse

    crow = lax.broadcasted_iota(jnp.int32, (cwindow, cz), 0) - 8
    clow = jnp.where(member_at > 0, -8, 0)
    chigh = jnp.where(member_at < members - 1, hy + 8, hy)
    within = jnp.where((crow >= clow) & (crow < chigh), SIXTH, 0.0)
    for region in range(3):
        alive = 1.0 if region == 1 else there(region - 1, 0).astype(f32)
        inside[region] = within * alive

    def wide_mask(rows):
        return lax.broadcasted_iota(jnp.int32, (rows, cz), 1) % 2 == 0

    with phase("load"):
        load_refined.wait()
        lane1 = lax.broadcasted_iota(jnp.int32, (1, cz), 1)
        boxes = refined_ref.shape[2]
        box = cz // boxes
        marks = jnp.zeros((1, cz), jnp.int32)
        for b in range(boxes):
            marks = jnp.where(lane1 // box == b, jnp.full((1, cz), refined_ref[0, 0, b], jnp.int32), marks)
        flags[1, 1, pl.ds(0, 1), :] = (marks == 1).astype(f32)
        load_source.wait()
        load_potential.wait()

    with phase("pack"):
        here = checker(cy, cz)
        smooth_own = jnp.broadcast_to(flags[1, 1, 0:1, :], (cy, cz)) > 0.5
        acc = [jnp.zeros((8, cz), f32)] * 4
        for a in range(px):
            s0, s1 = raw[0, 2 * a], raw[0, 2 * a + 1]
            v0, v1 = raw[1, 2 * a], raw[1, 2 * a + 1]
            both = s0 + s1
            acc = [acc[t] + sum(both[8 * u:8 * u + 8] for u in range(t, cy // 8, 4)) for t in range(4)]
            red_rhs = jnp.where(here, s0, s1)
            own_rhs[a] = red_rhs
            mix[HALO + a, own_rows, :] = jnp.where(smooth_own, red_rhs, jnp.where(here, v0, v1))
            black[HALO + a, own_rows, :] = jnp.where(here, v1, v0)
            black_rhs[HALO + a, own_rows, :] = jnp.where(here, s1, s0)
        acc = (acc[0] + acc[1]) + (acc[2] + acc[3])
        member_sums[0, pl.ds(0, 1), :] = jnp.sum(acc, axis=0, keepdims=True)

    with phase("barrier"):
        pl.semaphore_wait(barrier, expected)

    def report(g, carry):
        signal(ready, (g, member_at))
        return carry

    lax.fori_loop(0, group_at, report, 0)

    row = pl.ds(0, 1)

    def sum_copy(src, dst, n, at):
        return pltpu.make_async_remote_copy(
            src_ref=src, dst_ref=dst, send_sem=sum_sem.at[n], recv_sem=sum_sem.at[n + 1], device_id=at, device_id_type=MESH,
        )

    own_sum, plane_sum = member_sums.at[0, row], group_sums.at[0, row]
    no_sum = zeros.at[0, 0, row]

    def share_in_plane():
        for o in range(1, members):
            sum_copy(own_sum, member_sums.at[o, row], 0, (group_at, lax.rem(member_at + o, members))).start()

    def share_with_earlier():
        for o in range(groups - 1, 0, -1):
            @pl.when(group_at >= o)
            def _():
                for m in range(members):
                    sum_copy(own_sum, direct.at[o, pl.ds(member_at, 1)], 2, (group_at - o, m)).start()

    def fill_sums():
        for o in range(1, groups):
            @pl.when(group_at < o)
            def _():
                pltpu.make_async_copy(zeros.at[0, 0, pl.ds(0, members)], dummy.at[pl.ds(o * members, members)], sum_sem.at[2]).start()
                pltpu.make_async_copy(no_sum, group_sums.at[o, row], sum_sem.at[5]).start()

            @pl.when(group_at + o >= groups)
            def _():
                pltpu.make_async_copy(zeros.at[0, 0, pl.ds(0, members)], direct.at[o], sum_sem.at[3]).start()
                pltpu.make_async_copy(no_sum, dummy.at[pl.ds(groups * members + o, 1)], sum_sem.at[4]).start()

    def share_with_later():
        for o in range(1, groups):
            @pl.when(group_at + o < groups)
            def _():
                sum_copy(plane_sum, group_sums.at[o, row], 4, (group_at + o, member_at)).start()

    def sums(slots, n):
        return sum_copy(slots, slots, n, (group_at, member_at))

    in_plane = sums(member_sums.at[pl.ds(1, members - 1), row], 0)
    from_later = sums(direct.at[pl.ds(1, groups - 1)], 2)
    from_earlier = sums(group_sums.at[pl.ds(1, groups - 1), row], 4)

    def marks_round(n):
        dx, dy = SIDES[n]
        return 4, [(flags.at[1, 1, row], flags.at[1 - dx, 1 - dy, row])]

    def first_round(n):
        dx, dy = SIDES[n]
        pairs = []
        if dx and dy:
            pieces = ((0, 1, 0, 1, 4), (1, 1, 0, 1, 3), (2, 1, 0, 1, 2), (0, 1, 1, 2, 2), (1, 1, 1, 2, 1))
        elif dx:
            pieces = ((0, 1, 0, HALO, cy), (1, 2, 0, HALO - 1, cy))
        else:
            pieces = ((0, 1, 0, px, REACH + 1), (1, 1, 0, px, REACH), (2, 1, 0, px, REACH - 1))
        for kind, kinds, begin, end, deep in pieces:
            sx, tx = span(dx, begin, end, HALO, px)
            sy, ty = span(dy, 0, deep, ROW0, cy)
            pairs.append((field.at[pl.ds(kind, kinds), sx, sy], field.at[pl.ds(kind, kinds), tx, ty]))
        return (3 if dy else 0), pairs

    def second_coarse(n):
        dx, dy = SIDES[n]
        if dx and dy:
            pieces = ((0, 1, 5), (1, 2, 3), (2, 3, 1))
        elif dx:
            pieces = ((0, COARSE_HALO, hy),)
        else:
            pieces = ((0, hx, COARSE_REACH),)
        pairs = []
        for begin, end, deep in pieces:
            sx, tx = span(dx, begin, end, CPLANE0, hx)
            sy, ty = span(dy, 0, deep, CROW0, hy)
            pairs.append((mixed.at[sx, sy], mixed.at[tx, ty]))
        return 1, pairs

    def second_fine(n):
        dx, dy = SIDES[n]
        if dx and dy:
            pieces = ((0, 1, 0, 4), (1, 2, 0, 2))
        elif dx:
            pieces = ((0, HALO, 0, cy),)
        else:
            pieces = ((0, px, 1, REACH + 1),)
        pairs = []
        for begin, end, skip, deep in pieces:
            sx, tx = span(dx, begin, end, HALO, px)
            sy, ty = span(dy, skip, deep, ROW0, cy)
            pairs.append((mid.at[sx, sy], landed.at[tx, ty]))
        return 2, pairs

    def rows_of(pairs):
        total = 0
        for _, dst in pairs:
            total += functools.reduce(lambda p, q: p * q, dst.shape[:-1])
        return total

    odd = lax.rem(member_at, 2) == 1

    def start(round_of, order=(True, None, False)):
        for far in order:
            for n, (dx, dy) in enumerate(SIDES):
                if (dy == 0) != (far is None):
                    continue
                kind, pairs = round_of(n)
                now = there(dx, dy)
                if far is not None:
                    now = now & (odd if (dy > 0) == far else jnp.logical_not(odd))

                @pl.when(now)
                def _():
                    split = via and far and not dx and round_of is first_round
                    if split:
                        send_face(n)
                    for src, dst in () if split else pairs:
                        pltpu.make_async_remote_copy(
                            src_ref=src, dst_ref=dst, send_sem=send_sem.at[n], recv_sem=recv_sem.at[kind],
                            device_id=device(dx, dy), device_id_type=MESH,
                        ).start()

    around = px * DETOUR // 8
    via = members % 2 == 0
    detour = []
    at_row = 0
    for kind, deep in ((0, REACH + 1), (1, REACH), (2, REACH - 1)):
        detour.append((kind, deep, pl.ds(at_row, deep)))
        at_row += deep
    detour_rows = at_row * around
    direct_planes, around_planes = pl.ds(HALO, px - around), pl.ds(HALO + px - around, around)

    def send_face(n):
        dx, dy = SIDES[n]
        for by_detour in (True, False):
            for kind, deep, rows in detour:
                sy, ty = span(dy, 0, deep, ROW0, cy)
                planes = around_planes if by_detour else direct_planes
                pltpu.make_async_remote_copy(
                    src_ref=field.at[kind, planes, sy],
                    dst_ref=passing.at[pl.ds(0, around), rows] if by_detour else field.at[kind, planes, ty],
                    send_sem=send_sem.at[n], recv_sem=pass_sem.at[0] if by_detour else recv_sem.at[3],
                    device_id=device(0, 2 * dy if by_detour else dy), device_id_type=MESH,
                ).start()

    def passes(side):
        return (odd & (member_at >= 2)) if side < 0 else (jnp.logical_not(odd) & (member_at + 2 < members))

    def passed():
        part = dummy.at[pl.ds(0, detour_rows)]
        return pltpu.make_async_remote_copy(
            src_ref=part, dst_ref=part, send_sem=pass_sem.at[1], recv_sem=pass_sem.at[0],
            device_id=(group_at, member_at), device_id_type=MESH,
        )

    def pass_on(now):
        for side in (-1, 1):
            @pl.when(passes(side) & now)
            def _():
                passed().wait_recv()
                for kind, deep, rows in detour:
                    ty = span(-side, 0, deep, ROW0, cy)[1]
                    pltpu.make_async_remote_copy(
                        src_ref=passing.at[pl.ds(0, around), rows], dst_ref=field.at[kind, around_planes, ty],
                        send_sem=pass_sem.at[1], recv_sem=recv_sem.at[3],
                        device_id=device(0, side), device_id_type=MESH,
                    ).start()

    def fill(round_of):
        for n, (dx, dy) in enumerate(SIDES):
            kind, pairs = round_of(n)
            @pl.when(jnp.logical_not(there(-dx, -dy)))
            def _():
                for _, dst in pairs:
                    shape = dst.shape[:-1]
                    src = zeros.at[(0,) * (4 - len(dst.shape)) + tuple(pl.ds(0, size) for size in shape)]
                    pltpu.make_async_copy(src, dst, recv_sem.at[kind]).start()

    def all_of(rows, n, kind):
        part = dummy.at[pl.ds(0, rows)]
        return pltpu.make_async_remote_copy(
            src_ref=part, dst_ref=part, send_sem=send_sem.at[n], recv_sem=recv_sem.at[kind],
            device_id=(group_at, member_at), device_id_type=MESH,
        )

    def arrive(round_of, kind):
        arriving = (round_of(n) for n in range(len(SIDES)))
        all_of(sum(rows_of(pairs) for which, pairs in arriving if which == kind), 0, kind).wait_recv()

    def sent(*rounds):
        for n, (dx, dy) in enumerate(SIDES):
            rows = sum(rows_of(round_of(n)[1]) for round_of in rounds)

            @pl.when(there(dx, dy))
            def _():
                all_of(rows, n, 0).wait_send()

    with phase("start1"):
        share_in_plane()
        share_with_earlier()
        start(marks_round)
        start(first_round)
    with phase("fill"):
        fill_sums()
        for round_of in (marks_round, first_round, second_coarse, second_fine):
            fill(round_of)

    with phase("w_msum"):
        in_plane.wait_recv()
    part = member_sums[0, row, :]
    for o in range(1, members):
        part = part + member_sums[o, row, :]
    group_sums[0, row, :] = part
    if via:
        with phase("pass1"):
            pass_on(group_at < 2)
    with phase("w_ready"):
        @pl.when(group_at < groups - 1)
        def _():
            pl.semaphore_wait(ready, groups - 1 - group_at)
    share_with_later()
    if via:
        with phase("pass2"):
            pass_on(group_at >= 2)
    def plane_groups(t):
        wide_by = (REACH - t + 1) // 2
        for region, low, high in ((0, HALO - wide_by, HALO), (1, HALO, HALO + px), (2, HALO + px, HALO + px + wide_by)):
            for first in range(low, high, 4):
                yield region, range(first, min(first + 4, high))

    fine_mask = checker(window, cz)
    stages = ((mix, mix, black, red), (black_rhs, black, red, mid), (mix, red, mid, red), (black_rhs, mid, red, mid))

    with phase("w_marks"):
        arrive(marks_round, 4)
    with phase("masks"):
        edge = lax.broadcasted_iota(jnp.int32, (8, cz), 0) < REACH
        for x in range(3):
            low, own, high = flags[x, 0], flags[x, 1], flags[x, 2]
            low, own, high = (jnp.broadcast_to(v[0:1], (8, cz)) for v in (low, own, high))
            active[x, pl.ds(0, 8), :] = jnp.where(edge, low, own)
            for t in range(1, window // 8 - 1):
                active[x, pl.ds(8 * t, 8), :] = own
            active[x, pl.ds(window - 8, 8), :] = jnp.where(edge, own, high)

    with phase("unit"):
        rows = pl.ds(ROW0 - REACH, window)
        for p in range(HALO - 2, HALO + px + 2):
            region = 0 if p < HALO else 1 if p < HALO + px else 2
            unit_red[p, rows, :] = active[region] * SIXTH
        for t, other, out in ((1, unit_red, unit_black), (2, unit_black, unit_red)):
            for region, planes in plane_groups(t):
                weight = active[region] * SIXTH
                sums = neighbours(other, planes, ROW0 - REACH, window, t % 2, fine_mask, 1)
                for p, nbr in zip(planes, sums):
                    out[p, rows, :] = (1.0 + nbr) * weight

    with phase("w_along"):
        arrive(first_round, 0)
    with phase("inner"):
        inner = cy - 2
        inner_rows = pl.ds(ROW0 + 1, inner)
        at = lax.broadcasted_iota(jnp.int32, (inner, cz), 0)
        inner_mask = jnp.logical_not(checker(inner, cz))
        smoothed = [jnp.broadcast_to(flags[x, 1, row, :], (inner, cz)) > 0.5 for x in range(3)]
        for t, (right, old, other, out) in enumerate(stages[:-1]):
            reached = (at >= t) & (at < inner - t)
            for region, planes in plane_groups(t):
                keep = smoothed[region] & reached
                sums = neighbours(other, planes, ROW0 + 1, inner, t % 2, inner_mask, 1)
                for p, nbr in zip(planes, sums):
                    total = right[p, inner_rows, :] + nbr
                    out[p, inner_rows, :] = jnp.where(keep, total * SIXTH, old[p, inner_rows, :])

    with phase("w_gsum"):
        from_earlier.wait_recv()
    with phase("w_direct"):
        from_later.wait_recv()
    with phase("mean"):
        total = group_sums[0, row, :]
        later = jnp.zeros((members, cz), f32)
        for o in range(1, groups):
            total = total + group_sums[o, row, :]
            later = later + direct[o]
        total = total + jnp.sum(later, axis=0, keepdims=True)
        mean = jnp.sum(total) / (cx * cy * cz * groups * members)

    with phase("w_halo1"):
        arrive(first_round, 3)

    with phase("edges"):
        edge_mask = checker(8, cz)
        sub = lax.broadcasted_iota(jnp.int32, (8, cz), 0)
        for t, (right, old, other, out) in enumerate(stages[:-1]):
            for region, planes in plane_groups(t):
                for low in (True, False):
                    first = ROW0 - REACH if low else ROW0 + cy - REACH
                    rows = pl.ds(first, 8)
                    keep = active[region, pl.ds(first - ROW0 + REACH, 8), :] > 0.5
                    fresh = (sub <= REACH + t) if low else (sub >= REACH - 1 - t)
                    sums = neighbours(other, planes, first, 8, t % 2, edge_mask, 1)
                    for p, nbr in zip(planes, sums):
                        total = right[p, rows, :] + nbr
                        value = jnp.where(keep, total * SIXTH, old[p, rows, :])
                        out[p, rows, :] = jnp.where(fresh, value, out[p, rows, :])

    def black_sweep(right, other, out):
        rows = pl.ds(ROW0 - REACH, window)
        for region, planes in plane_groups(REACH - 1):
            keep = active[region] > 0.5
            sums = neighbours(other, planes, ROW0 - REACH, window, 1, fine_mask, 1)
            for p, nbr in zip(planes, sums):
                total = right[p, rows, :] - mean + nbr
                before = out[p, rows, :]
                out[p, rows, :] = jnp.where(keep, total * SIXTH, before)
                if region == 1:
                    defect[p - HALO] = jnp.where(keep, 0.0, total - 6.0 * before)

    with phase("last_pre"):
        rows = pl.ds(ROW0 - REACH, window)
        for p in range(HALO - 1, HALO + px + 1):
            red[p, rows, :] = red[p, rows, :] - mean * unit_red[p, rows, :]
        black_sweep(black_rhs, red, mid)

    own_mask = checker(cy, cz)

    def red_defects(other, planes):
        sums = neighbours(other, [HALO + a for a in planes], ROW0, cy, 0, own_mask, 1)
        for a, nbr in zip(planes, sums):
            centre = red[HALO + a, own_rows, :]
            yield a, centre, own_rhs[a] - mean + nbr - 6.0 * centre

    with phase("restrict"):
        for first in range(0, px, 4):
            for a, centre, res in red_defects(mid, range(first, first + 4)):
                pair_rows[a] = res + defect[a, pl.ds(REACH, cy), :]
        chosen, even = checker(hy, cz, 2), wide_mask(hy)
        for a in range(hx):
            first, second = (
                pair_rows[2 * a + k, pl.ds(0, hy, stride=2), :] + pair_rows[2 * a + k, pl.ds(1, hy, stride=2), :]
                for k in range(2)
            )
            zero, one = jnp.where(chosen, first, second), jnp.where(chosen, second, first)
            both = jnp.where(even, zero + pltpu.roll(zero, cz - 1, 1), one + pltpu.roll(one, 1, 1))
            mixed[CPLANE0 + a, pl.ds(CROW0, hy), :] = 0.5 * both

    with phase("start2"):
        start(second_coarse)
        start(second_fine, (False, None, True))
        for a in range(px):
            own_rhs[a] = own_rhs[a] - mean
    with phase("w_coarse"):
        arrive(second_coarse, 1)

    with phase("coarse"):
        coarse_rows = pl.ds(CROW0 - 8, cwindow)
        coarse_even = wide_mask(cwindow)
        coarse_mask = checker(cwindow, cz, 2)

        def regions(wide_by):
            first, last = CPLANE0, CPLANE0 + hx
            return (0, first - wide_by, first), (1, first, last), (2, last, last + wide_by)

        for region, low, high in regions(COARSE_HALO):
            weight = inside[region]
            for a in range(low, high):
                both = mixed[a, coarse_rows, :]
                s0 = jnp.where(coarse_even, both, pltpu.roll(both, 1, 1))
                rhs0[a, coarse_rows, :] = s0
                rhs1[a, coarse_rows, :] = jnp.where(coarse_even, pltpu.roll(both, cz - 1, 1), both)
                corr0[a, coarse_rows, :] = s0 * weight
        for t in range(1, 2 * COARSE):
            right, other, out = (rhs1, corr0, corr1) if t % 2 else (rhs0, corr1, corr0)
            for region, low, high in regions((COARSE_REACH - t + 1) // 2):
                weight = inside[region]
                for first in range(low, high, 4):
                    planes = range(first, min(first + 4, high))
                    sums = neighbours(other, planes, CROW0 - 8, cwindow, t % 2, coarse_mask, 2)
                    for a, nbr in zip(planes, sums):
                        out[a, coarse_rows, :] = (right[a, coarse_rows, :] + nbr) * weight

    with phase("w_fine2"):
        arrive(second_fine, 2)

    with phase("prolong"):
        half_rows = hy + 8
        rows = pl.ds(CROW0 - 4, half_rows)
        pick = checker(half_rows, cz, 2)
        low_rows, high_rows = pl.ds(ROW0 - 8, 8), pl.ds(ROW0 + cy, 8)
        sub = lax.broadcasted_iota(jnp.int32, (8, cz), 0)
        for p in range(px + 2 * HALO):
            a, k = CPLANE0 + (p - HALO) // 2, (p - HALO) % 2
            c0, c1 = corr0[a, rows, :], corr1[a, rows, :]
            plane = jnp.where(pick, c1, c0) if k else jnp.where(pick, c0, c1)
            wide[p, pl.ds(0, half_rows, stride=2), :] = plane
            wide[p, pl.ds(1, half_rows, stride=2), :] = plane
        for p in range(px + 2 * HALO):
            low, own, high = wide[p, pl.ds(0, 8), :], wide[p, pl.ds(8, cy), :], wide[p, pl.ds(8 + cy, 8), :]
            if HALO <= p < HALO + px:
                post[p, own_rows, :] = mid[p, own_rows, :] + own
                post[p, low_rows, :] = jnp.where(sub == 7, mid[p, low_rows, :], landed[p, low_rows, :]) + low
                post[p, high_rows, :] = jnp.where(sub == 0, mid[p, high_rows, :], landed[p, high_rows, :]) + high
            else:
                post[p, own_rows, :] = landed[p, own_rows, :] + own
                post[p, low_rows, :] = landed[p, low_rows, :] + low
                post[p, high_rows, :] = landed[p, high_rows, :] + high
            if 1 <= p < px + 2 * HALO - 1:
                red[p, own_rows, :] = red[p, own_rows, :] + own
                red[p, low_rows, :] = red[p, low_rows, :] + low
                red[p, high_rows, :] = red[p, high_rows, :] + high

    with phase("post"):
        rows = pl.ds(ROW0 - REACH, window)
        for t in range(REACH - 1):
            right, other, out = (black_rhs, red, post) if t % 2 else (mix, post, red)
            for region, planes in plane_groups(t):
                keep = active[region] > 0.5
                sums = neighbours(other, planes, ROW0 - REACH, window, t % 2, fine_mask, 1)
                for p, nbr in zip(planes, sums):
                    total = right[p, rows, :] - mean + nbr
                    out[p, rows, :] = jnp.where(keep, total * SIXTH, out[p, rows, :])
        black_sweep(black_rhs, red, post)

    with phase("w_sent"):
        sent(marks_round, first_round, second_coarse, second_fine)
        if via:
            for side in (-1, 1):
                @pl.when(passes(side))
                def _():
                    passed().wait_send()
        in_plane.wait_send()
        from_later.wait_send()
        from_earlier.wait_send()


def put(red, post, defect, contrast, smoothed_out, residual_out, smoothed, residual, sem):
    px, cy, cz = contrast.shape
    own_rows = pl.ds(ROW0, cy)
    mask = checker(cy, cz)
    copies = []

    def send(n, src, dst, first, size):
        part = pl.ds(2 * first, 2 * size)
        copies.append(pltpu.make_async_copy(src.at[part], dst.at[part], sem.at[n]))
        copies[-1].start()

    for a in range(px):
        centre, value = red[HALO + a, own_rows, :], post[HALO + a, own_rows, :]
        smoothed[2 * a] = jnp.where(mask, centre, value)
        smoothed[2 * a + 1] = jnp.where(mask, value, centre)
    send(0, smoothed, smoothed_out, 0, px)
    size = px // PIECES
    for piece in range(PIECES):
        planes = range(piece * size, (piece + 1) * size)
        sums = neighbours(post, [HALO + a for a in planes], ROW0, cy, 0, mask, 1)
        for a, nbr in zip(planes, sums):
            res, other = contrast[a] + nbr - 6.0 * red[HALO + a, own_rows, :], defect[a, pl.ds(REACH, cy), :]
            residual[2 * a] = jnp.where(mask, res, other)
            residual[2 * a + 1] = jnp.where(mask, other, res)
        send(1 + piece, residual, residual_out, piece * size, size)
    for c in copies:
        c.wait()


def per_device(dims, source, potential, refined):
    cx, cy, cz = source.shape
    groups, members = dims
    px, hx, hy = cx // 2, cx // 4, cy // 2
    fine = (px + 2 * HALO, ROW0 + cy + ROW0, cz)
    coarse = (hx + 2 * CPLANE0, hy + 2 * CROW0, cz)
    f32 = jnp.float32
    dma = pltpu.SemaphoreType.DMA
    any_spec = pl.BlockSpec(memory_space=pl.ANY)
    vmem_spec = pl.BlockSpec(memory_space=pltpu.VMEM)
    results = pl.pallas_call(
        functools.partial(kernel, dims, (cx, cy, cz)),
        out_shape=[
            pltpu.VMEM(fine, f32),
            pltpu.VMEM(fine, f32),
            pltpu.VMEM((px, cy + 2 * REACH, cz), f32),
            pltpu.VMEM((px, cy, cz), f32),
        ],
        in_specs=[any_spec] * 3,
        out_specs=[vmem_spec] * 4,
        scratch_shapes=[
            pltpu.SMEM(refined.shape, jnp.int32),
            pltpu.VMEM((2, cx, cy, cz), f32),
            pltpu.VMEM((3, *fine), f32),
            pltpu.VMEM(fine, f32),
            pltpu.VMEM(fine, f32),
            pltpu.VMEM((px, cy, cz), f32),
            pltpu.VMEM(coarse, f32),
            pltpu.VMEM(coarse, f32),
            pltpu.VMEM(coarse, f32),
            pltpu.VMEM(coarse, f32),
            pltpu.VMEM(coarse, f32),
            pltpu.VMEM((px + 2 * HALO, cy + 16, cz), f32),
            pltpu.VMEM((3, 3, 8, cz), f32),
            pltpu.VMEM((3, cy + 2 * REACH, cz), f32),
            pltpu.VMEM((3, hy + 16, cz), f32),
            pltpu.VMEM((members, 8, cz), f32),
            pltpu.VMEM((groups, 8, cz), f32),
            pltpu.VMEM((groups, members, cz), f32),
            pltpu.VMEM((px, 16, cz), f32),
            pltpu.VMEM(fine, f32),
            pltpu.VMEM(fine, f32),
            pltpu.VMEM((2, px, cy, cz), f32),
            pltpu.VMEM((64 * cy, cz), f32),
            dma((3,)),
            dma((len(SIDES),)),
            dma((5,)),
            dma((6,)),
            dma((2,)),
            pltpu.SemaphoreType.REGULAR,
        ],
        compiler_params=pltpu.CompilerParams(collective_id=0, has_side_effects=True),
    )(refined, source, potential)
    return tuple(pl.pallas_call(
        put,
        out_shape=[jax.ShapeDtypeStruct(source.shape, f32)] * 2,
        in_specs=[vmem_spec] * 4,
        out_specs=[any_spec] * 2,
        scratch_shapes=[pltpu.VMEM(source.shape, f32), pltpu.VMEM(source.shape, f32), dma((1 + PIECES,))],
    )(*(pltpu.with_memory_space_constraint(v, pltpu.VMEM) for v in results)))


def solution(mesh):
    spec = P("group", "member", None)
    return jax.shard_map(
        functools.partial(per_device, (mesh.shape["group"], mesh.shape["member"])),
        mesh=mesh,
        in_specs=(spec, spec, spec),
        out_specs=(spec, spec),
        check_vma=False,
    )
```

```python
import contextlib
import functools

import jax
import jax.numpy as jnp
from jax import lax
from jax.experimental import pallas as pl
from jax.experimental.pallas import tpu as pltpu
from jax.sharding import PartitionSpec as P

SWEEPS = 2
COARSE = 2
REACH = 2 * SWEEPS
HALO = (REACH + 2) // 2
COARSE_REACH = 2 * COARSE - 1 + (REACH + 2) // 2
COARSE_HALO = COARSE_REACH // 2
ROW0 = 8 + REACH
CROW0 = 16
CPLANE0 = COARSE_HALO + 1
SIDES = ((0, -1), (0, 1), (-1, 0), (1, 0), (-1, -1), (-1, 1), (1, -1), (1, 1))
MESH = pl.DeviceIdType.MESH
SIXTH = 1.0 / 6.0
DETOUR = 3
PIECES = 4


def phase(name):
    return contextlib.nullcontext()


def span(side, begin, end, first, count):
    if side == 0:
        return pl.ds(first, count), pl.ds(first, count)
    if side > 0:
        return pl.ds(first + count - end, end - begin), pl.ds(first - end, end - begin)
    return pl.ds(first + begin, end - begin), pl.ds(first + count + begin, end - begin)


def checker(rows, cz, lanes_per=1):
    r = lax.broadcasted_iota(jnp.int32, (rows, cz), 0)
    return ((r + lax.broadcasted_iota(jnp.int32, (rows, cz), 1) // lanes_per) & 1) == 0


def lanes(value, step):
    cz = value.shape[1]
    lane = lax.broadcasted_iota(jnp.int32, value.shape, 1)
    low = jnp.where(lane < step, 0.0, pltpu.roll(value, step, 1))
    high = jnp.where(lane >= cz - step, 0.0, pltpu.roll(value, cz - step, 1))
    return low + high


def neighbours(other, planes, row, rows, colour, mask, step):
    centres = {}
    out = []
    for p in planes:
        for q in (p - 1, p, p + 1):
            if q not in centres:
                centres[q] = other[q, pl.ds(row, rows), :]
        near, far = (centres[p - 1], centres[p + 1]) if colour == 0 else (centres[p + 1], centres[p - 1])
        total = centres[p] + jnp.where(mask, near, far)
        total = total + (other[p, pl.ds(row - 1, rows), :] + other[p, pl.ds(row + 1, rows), :])
        out.append(total + lanes(centres[p], step))
    return out


def kernel(
    dims, sizes,
    refined_hbm, source_ref, potential_ref,
    red, post, defect, own_rhs,
    refined_ref, raw, field, mid, landed, pair_rows, mixed, rhs0, rhs1, corr0, corr1, wide,
    flags, active, inside, member_sums, group_sums, direct, passing, unit_red, unit_black, zeros, dummy,
    local_sem, send_sem, recv_sem, sum_sem, pass_sem, ready,
):
    groups, members = dims
    cx, cy, cz = sizes
    px, hx, hy = cx // 2, cx // 4, cy // 2
    group_at = lax.axis_index("group")
    member_at = lax.axis_index("member")
    f32 = jnp.float32
    black, mix, black_rhs = field.at[0], field.at[1], field.at[2]
    own_rows = pl.ds(ROW0, cy)
    window = cy + 2 * REACH
    cwindow = hy + 16

    load_source = pltpu.make_async_copy(source_ref, raw.at[0], local_sem.at[0])
    load_potential = pltpu.make_async_copy(potential_ref, raw.at[1], local_sem.at[1])
    load_refined = pltpu.make_async_copy(refined_hbm, refined_ref, local_sem.at[2])
    load_source.start()
    load_potential.start()
    load_refined.start()

    def there(dx, dy):
        ok = None
        for side, at, count in ((dx, group_at, groups), (dy, member_at, members)):
            if side == 0:
                continue
            here = at > 0 if side < 0 else at < count - 1
            ok = here if ok is None else ok & here
        return ok

    def device(dx, dy):
        return (group_at + dx, member_at + dy)

    def signal(sem, at):
        pl.semaphore_signal(sem, inc=1, device_id=at, device_id_type=MESH)

    barrier = pltpu.get_barrier_semaphore()
    for o in range(1, members):
        signal(barrier, (group_at, lax.rem(member_at + o, members)))
    expected = jnp.int32(members - 1) + group_at * members
    for dy in (-1, 0, 1):
        @pl.when(there(-1, dy))
        def _():
            signal(barrier, device(-1, dy))
        expected = expected + there(1, dy).astype(jnp.int32)

    def greet(o, carry):
        for m in range(members):
            signal(barrier, (group_at + o, m))
        return carry

    lax.fori_loop(1, groups - group_at, greet, 0)

    blank_rows = jnp.zeros((cy, cz), f32)
    for kind in range(2):
        for p in range(px):
            zeros[kind, p] = blank_rows
    blank_coarse = jnp.zeros((cwindow, cz), f32)
    for a in range(hx + 2 * CPLANE0):
        mixed[a, pl.ds(CROW0 - 8, cwindow), :] = blank_coarse
    for a in (0, hx + 2 * CPLANE0 - 1):
        corr0[a, pl.ds(CROW0 - 8, cwindow), :] = blank_coarse

    crow = lax.broadcasted_iota(jnp.int32, (cwindow, cz), 0) - 8
    clow = jnp.where(member_at > 0, -8, 0)
    chigh = jnp.where(member_at < members - 1, hy + 8, hy)
    within = jnp.where((crow >= clow) & (crow < chigh), SIXTH, 0.0)
    for region in range(3):
        alive = 1.0 if region == 1 else there(region - 1, 0).astype(f32)
        inside[region] = within * alive

    def wide_mask(rows):
        return lax.broadcasted_iota(jnp.int32, (rows, cz), 1) % 2 == 0

    with phase("load"):
        load_refined.wait()
        lane1 = lax.broadcasted_iota(jnp.int32, (1, cz), 1)
        boxes = refined_ref.shape[2]
        box = cz // boxes
        marks = jnp.zeros((1, cz), jnp.int32)
        for b in range(boxes):
            marks = jnp.where(lane1 // box == b, jnp.full((1, cz), refined_ref[0, 0, b], jnp.int32), marks)
        flags[1, 1, pl.ds(0, 1), :] = (marks == 1).astype(f32)
        load_source.wait()
        load_potential.wait()

    with phase("pack"):
        here = checker(cy, cz)
        smooth_own = jnp.broadcast_to(flags[1, 1, 0:1, :], (cy, cz)) > 0.5
        acc = [jnp.zeros((8, cz), f32)] * 4
        for a in range(px):
            s0, s1 = raw[0, 2 * a], raw[0, 2 * a + 1]
            v0, v1 = raw[1, 2 * a], raw[1, 2 * a + 1]
            both = s0 + s1
            acc = [acc[t] + sum(both[8 * u:8 * u + 8] for u in range(t, cy // 8, 4)) for t in range(4)]
            red_rhs = jnp.where(here, s0, s1)
            own_rhs[a] = red_rhs
            mix[HALO + a, own_rows, :] = jnp.where(smooth_own, red_rhs, jnp.where(here, v0, v1))
            black[HALO + a, own_rows, :] = jnp.where(here, v1, v0)
            black_rhs[HALO + a, own_rows, :] = jnp.where(here, s1, s0)
        acc = (acc[0] + acc[1]) + (acc[2] + acc[3])
        member_sums[0, pl.ds(0, 1), :] = jnp.sum(acc, axis=0, keepdims=True)

    with phase("barrier"):
        pl.semaphore_wait(barrier, expected)

    def report(g, carry):
        signal(ready, (g, member_at))
        return carry

    lax.fori_loop(0, group_at, report, 0)

    row = pl.ds(0, 1)

    def sum_copy(src, dst, n, at):
        return pltpu.make_async_remote_copy(
            src_ref=src, dst_ref=dst, send_sem=sum_sem.at[0], recv_sem=sum_sem.at[n], device_id=at, device_id_type=MESH,
        )

    own_sum, plane_sum = member_sums.at[0, row], group_sums.at[0, row]
    no_sum = zeros.at[0, 0, row]

    def share_in_plane():
        for o in range(1, members):
            sum_copy(own_sum, member_sums.at[o, row], 1, (group_at, lax.rem(member_at + o, members))).start()

    def share_with_earlier():
        for o in range(groups - 1, 0, -1):
            @pl.when(group_at >= o)
            def _():
                for m in range(members):
                    sum_copy(own_sum, direct.at[o, pl.ds(member_at, 1)], 2, (group_at - o, m)).start()

    def fill_sums():
        for o in range(1, groups):
            @pl.when(group_at < o)
            def _():
                pltpu.make_async_copy(zeros.at[0, 0, pl.ds(0, members)], dummy.at[pl.ds(o * members, members)], sum_sem.at[0]).start()
                pltpu.make_async_copy(no_sum, group_sums.at[o, row], sum_sem.at[3]).start()

            @pl.when(group_at + o >= groups)
            def _():
                pltpu.make_async_copy(zeros.at[0, 0, pl.ds(0, members)], direct.at[o], sum_sem.at[2]).start()
                pltpu.make_async_copy(no_sum, dummy.at[pl.ds(groups * members + o, 1)], sum_sem.at[0]).start()

    def share_with_later():
        for o in range(1, groups):
            @pl.when(group_at + o < groups)
            def _():
                sum_copy(plane_sum, group_sums.at[o, row], 3, (group_at + o, member_at)).start()

    def sums(slots, n):
        return sum_copy(slots, slots, n, (group_at, member_at))

    in_plane = sums(member_sums.at[pl.ds(1, members - 1), row], 1)
    from_later = sums(direct.at[pl.ds(1, groups - 1)], 2)
    from_earlier = sums(group_sums.at[pl.ds(1, groups - 1), row], 3)
    all_sums = sums(dummy.at[pl.ds(0, members - 1 + (groups - 1) * (members + 1))], 1)

    def marks_round(n):
        dx, dy = SIDES[n]
        return 4, [(flags.at[1, 1, row], flags.at[1 - dx, 1 - dy, row])]

    def first_round(n):
        dx, dy = SIDES[n]
        pairs = []
        if dx and dy:
            pieces = ((0, 1, 0, 1, 4), (1, 1, 0, 1, 3), (2, 1, 0, 1, 2), (0, 1, 1, 2, 2), (1, 1, 1, 2, 1))
        elif dx:
            pieces = ((0, 1, 0, HALO, cy), (1, 2, 0, HALO - 1, cy))
        else:
            pieces = ((0, 1, 0, px, REACH + 1), (1, 1, 0, px, REACH), (2, 1, 0, px, REACH - 1))
        for kind, kinds, begin, end, deep in pieces:
            sx, tx = span(dx, begin, end, HALO, px)
            sy, ty = span(dy, 0, deep, ROW0, cy)
            pairs.append((field.at[pl.ds(kind, kinds), sx, sy], field.at[pl.ds(kind, kinds), tx, ty]))
        return (3 if dy else 0), pairs

    def second_coarse(n):
        dx, dy = SIDES[n]
        if dx and dy:
            pieces = ((0, 1, 5), (1, 2, 3), (2, 3, 1))
        elif dx:
            pieces = ((0, COARSE_HALO, hy),)
        else:
            pieces = ((0, hx, COARSE_REACH),)
        pairs = []
        for begin, end, deep in pieces:
            sx, tx = span(dx, begin, end, CPLANE0, hx)
            sy, ty = span(dy, 0, deep, CROW0, hy)
            pairs.append((mixed.at[sx, sy], mixed.at[tx, ty]))
        return 1, pairs

    def second_fine(n):
        dx, dy = SIDES[n]
        if dx and dy:
            pieces = ((0, 1, 0, 4), (1, 2, 0, 2))
        elif dx:
            pieces = ((0, HALO, 0, cy),)
        else:
            pieces = ((0, px, 1, REACH + 1),)
        pairs = []
        for begin, end, skip, deep in pieces:
            sx, tx = span(dx, begin, end, HALO, px)
            sy, ty = span(dy, skip, deep, ROW0, cy)
            pairs.append((mid.at[sx, sy], landed.at[tx, ty]))
        return 2, pairs

    def rows_of(pairs):
        total = 0
        for _, dst in pairs:
            total += functools.reduce(lambda p, q: p * q, dst.shape[:-1])
        return total

    odd = lax.rem(member_at, 2) == 1

    def start(round_of, order=(True, None, False)):
        for far in order:
            for n, (dx, dy) in enumerate(SIDES):
                if (dy == 0) != (far is None):
                    continue
                kind, pairs = round_of(n)
                now = there(dx, dy)
                if far is not None:
                    now = now & (odd if (dy > 0) == far else jnp.logical_not(odd))

                @pl.when(now)
                def _():
                    split = via and far and not dx and round_of is first_round
                    if split:
                        send_face(n)
                    for src, dst in () if split else pairs:
                        pltpu.make_async_remote_copy(
                            src_ref=src, dst_ref=dst, send_sem=send_sem.at[n], recv_sem=recv_sem.at[kind],
                            device_id=device(dx, dy), device_id_type=MESH,
                        ).start()

    around = px * DETOUR // 8
    via = members % 2 == 0
    detour = []
    at_row = 0
    for kind, deep in ((0, REACH + 1), (1, REACH), (2, REACH - 1)):
        detour.append((kind, deep, pl.ds(at_row, deep)))
        at_row += deep
    detour_rows = at_row * around
    direct_planes, around_planes = pl.ds(HALO, px - around), pl.ds(HALO + px - around, around)

    def send_face(n):
        dx, dy = SIDES[n]
        for by_detour in (True, False):
            for kind, deep, rows in detour:
                sy, ty = span(dy, 0, deep, ROW0, cy)
                planes = around_planes if by_detour else direct_planes
                pltpu.make_async_remote_copy(
                    src_ref=field.at[kind, planes, sy],
                    dst_ref=passing.at[pl.ds(0, around), rows] if by_detour else field.at[kind, planes, ty],
                    send_sem=send_sem.at[n], recv_sem=pass_sem.at[0] if by_detour else recv_sem.at[3],
                    device_id=device(0, 2 * dy if by_detour else dy), device_id_type=MESH,
                ).start()

    def passes(side):
        return (odd & (member_at >= 2)) if side < 0 else (jnp.logical_not(odd) & (member_at + 2 < members))

    def passed():
        part = dummy.at[pl.ds(0, detour_rows)]
        return pltpu.make_async_remote_copy(
            src_ref=part, dst_ref=part, send_sem=pass_sem.at[1], recv_sem=pass_sem.at[0],
            device_id=(group_at, member_at), device_id_type=MESH,
        )

    def pass_on(now):
        for side in (-1, 1):
            @pl.when(passes(side) & now)
            def _():
                passed().wait_recv()
                for kind, deep, rows in detour:
                    ty = span(-side, 0, deep, ROW0, cy)[1]
                    pltpu.make_async_remote_copy(
                        src_ref=passing.at[pl.ds(0, around), rows], dst_ref=field.at[kind, around_planes, ty],
                        send_sem=pass_sem.at[1], recv_sem=recv_sem.at[3],
                        device_id=device(0, side), device_id_type=MESH,
                    ).start()

    def fill(round_of):
        for n, (dx, dy) in enumerate(SIDES):
            kind, pairs = round_of(n)
            @pl.when(jnp.logical_not(there(-dx, -dy)))
            def _():
                for _, dst in pairs:
                    shape = dst.shape[:-1]
                    src = zeros.at[(0,) * (4 - len(dst.shape)) + tuple(pl.ds(0, size) for size in shape)]
                    pltpu.make_async_copy(src, dst, recv_sem.at[kind]).start()

    def all_of(rows, n, kind):
        part = dummy.at[pl.ds(0, rows)]
        return pltpu.make_async_remote_copy(
            src_ref=part, dst_ref=part, send_sem=send_sem.at[n], recv_sem=recv_sem.at[kind],
            device_id=(group_at, member_at), device_id_type=MESH,
        )

    def arrive(round_of, kind):
        arriving = (round_of(n) for n in range(len(SIDES)))
        all_of(sum(rows_of(pairs) for which, pairs in arriving if which == kind), 0, kind).wait_recv()

    def sent(*rounds):
        for n, (dx, dy) in enumerate(SIDES):
            rows = sum(rows_of(round_of(n)[1]) for round_of in rounds)

            @pl.when(there(dx, dy))
            def _():
                all_of(rows, n, 0).wait_send()

    with phase("start1"):
        share_in_plane()
        share_with_earlier()
        start(marks_round)
        start(first_round)
    with phase("fill"):
        fill_sums()
        for round_of in (marks_round, first_round, second_coarse, second_fine):
            fill(round_of)

    with phase("w_msum"):
        in_plane.wait_recv()
    part = member_sums[0, row, :]
    for o in range(1, members):
        part = part + member_sums[o, row, :]
    group_sums[0, row, :] = part
    if via:
        with phase("pass1"):
            pass_on(group_at < 2)
    with phase("w_ready"):
        @pl.when(group_at < groups - 1)
        def _():
            pl.semaphore_wait(ready, groups - 1 - group_at)
    share_with_later()
    if via:
        with phase("pass2"):
            pass_on(group_at >= 2)
    def plane_groups(t):
        wide_by = (REACH - t + 1) // 2
        for region, low, high in ((0, HALO - wide_by, HALO), (1, HALO, HALO + px), (2, HALO + px, HALO + px + wide_by)):
            for first in range(low, high, 4):
                yield region, range(first, min(first + 4, high))

    fine_mask = checker(window, cz)
    stages = ((mix, mix, black, red), (black_rhs, black, red, mid), (mix, red, mid, red), (black_rhs, mid, red, mid))

    with phase("w_marks"):
        arrive(marks_round, 4)
    with phase("masks"):
        edge = lax.broadcasted_iota(jnp.int32, (8, cz), 0) < REACH
        for x in range(3):
            low, own, high = flags[x, 0], flags[x, 1], flags[x, 2]
            low, own, high = (jnp.broadcast_to(v[0:1], (8, cz)) for v in (low, own, high))
            active[x, pl.ds(0, 8), :] = jnp.where(edge, low, own)
            for t in range(1, window // 8 - 1):
                active[x, pl.ds(8 * t, 8), :] = own
            active[x, pl.ds(window - 8, 8), :] = jnp.where(edge, own, high)

    with phase("unit"):
        rows = pl.ds(ROW0 - REACH, window)
        for p in range(HALO - 2, HALO + px + 2):
            region = 0 if p < HALO else 1 if p < HALO + px else 2
            unit_red[p, rows, :] = active[region] * SIXTH
        for t, other, out in ((1, unit_red, unit_black), (2, unit_black, unit_red)):
            for region, planes in plane_groups(t):
                weight = active[region] * SIXTH
                sums = neighbours(other, planes, ROW0 - REACH, window, t % 2, fine_mask, 1)
                for p, nbr in zip(planes, sums):
                    out[p, rows, :] = (1.0 + nbr) * weight

    with phase("w_along"):
        arrive(first_round, 0)
    with phase("inner"):
        inner = cy - 2
        inner_rows = pl.ds(ROW0 + 1, inner)
        at = lax.broadcasted_iota(jnp.int32, (inner, cz), 0)
        inner_mask = jnp.logical_not(checker(inner, cz))
        smoothed = [jnp.broadcast_to(flags[x, 1, row, :], (inner, cz)) > 0.5 for x in range(3)]
        for t, (right, old, other, out) in enumerate(stages[:-1]):
            reached = (at >= t) & (at < inner - t)
            for region, planes in plane_groups(t):
                keep = smoothed[region] & reached
                sums = neighbours(other, planes, ROW0 + 1, inner, t % 2, inner_mask, 1)
                for p, nbr in zip(planes, sums):
                    total = right[p, inner_rows, :] + nbr
                    out[p, inner_rows, :] = jnp.where(keep, total * SIXTH, old[p, inner_rows, :])

    with phase("w_gsum"):
        from_earlier.wait_recv()
    with phase("w_direct"):
        from_later.wait_recv()
    with phase("mean"):
        total = group_sums[0, row, :]
        later = jnp.zeros((members, cz), f32)
        for o in range(1, groups):
            total = total + group_sums[o, row, :]
            later = later + direct[o]
        total = total + jnp.sum(later, axis=0, keepdims=True)
        mean = jnp.sum(total) / (cx * cy * cz * groups * members)

    with phase("w_halo1"):
        arrive(first_round, 3)

    with phase("edges"):
        edge_mask = checker(8, cz)
        sub = lax.broadcasted_iota(jnp.int32, (8, cz), 0)
        for t, (right, old, other, out) in enumerate(stages[:-1]):
            for region, planes in plane_groups(t):
                for low in (True, False):
                    first = ROW0 - REACH if low else ROW0 + cy - REACH
                    rows = pl.ds(first, 8)
                    keep = active[region, pl.ds(first - ROW0 + REACH, 8), :] > 0.5
                    fresh = (sub <= REACH + t) if low else (sub >= REACH - 1 - t)
                    sums = neighbours(other, planes, first, 8, t % 2, edge_mask, 1)
                    for p, nbr in zip(planes, sums):
                        total = right[p, rows, :] + nbr
                        value = jnp.where(keep, total * SIXTH, old[p, rows, :])
                        out[p, rows, :] = jnp.where(fresh, value, out[p, rows, :])

    def black_sweep(right, other, out):
        rows = pl.ds(ROW0 - REACH, window)
        for region, planes in plane_groups(REACH - 1):
            keep = active[region] > 0.5
            sums = neighbours(other, planes, ROW0 - REACH, window, 1, fine_mask, 1)
            for p, nbr in zip(planes, sums):
                total = right[p, rows, :] - mean + nbr
                before = out[p, rows, :]
                out[p, rows, :] = jnp.where(keep, total * SIXTH, before)
                if region == 1:
                    defect[p - HALO] = jnp.where(keep, 0.0, total - 6.0 * before)

    with phase("last_pre"):
        rows = pl.ds(ROW0 - REACH, window)
        for p in range(HALO - 1, HALO + px + 1):
            red[p, rows, :] = red[p, rows, :] - mean * unit_red[p, rows, :]
        black_sweep(black_rhs, red, mid)

    own_mask = checker(cy, cz)

    def red_defects(other, planes):
        sums = neighbours(other, [HALO + a for a in planes], ROW0, cy, 0, own_mask, 1)
        for a, nbr in zip(planes, sums):
            centre = red[HALO + a, own_rows, :]
            yield a, centre, own_rhs[a] - mean + nbr - 6.0 * centre

    with phase("restrict"):
        for first in range(0, px, 4):
            for a, centre, res in red_defects(mid, range(first, first + 4)):
                pair_rows[a] = res + defect[a, pl.ds(REACH, cy), :]
        chosen, even = checker(hy, cz, 2), wide_mask(hy)
        for a in range(hx):
            first, second = (
                pair_rows[2 * a + k, pl.ds(0, hy, stride=2), :] + pair_rows[2 * a + k, pl.ds(1, hy, stride=2), :]
                for k in range(2)
            )
            zero, one = jnp.where(chosen, first, second), jnp.where(chosen, second, first)
            both = jnp.where(even, zero + pltpu.roll(zero, cz - 1, 1), one + pltpu.roll(one, 1, 1))
            mixed[CPLANE0 + a, pl.ds(CROW0, hy), :] = 0.5 * both

    with phase("start2"):
        start(second_coarse)
        start(second_fine, (False, None, True))
        for a in range(px):
            own_rhs[a] = own_rhs[a] - mean
    with phase("w_coarse"):
        arrive(second_coarse, 1)

    with phase("coarse"):
        coarse_rows = pl.ds(CROW0 - 8, cwindow)
        coarse_even = wide_mask(cwindow)
        coarse_mask = checker(cwindow, cz, 2)

        def regions(wide_by):
            first, last = CPLANE0, CPLANE0 + hx
            return (0, first - wide_by, first), (1, first, last), (2, last, last + wide_by)

        for region, low, high in regions(COARSE_HALO):
            weight = inside[region]
            for a in range(low, high):
                both = mixed[a, coarse_rows, :]
                s0 = jnp.where(coarse_even, both, pltpu.roll(both, 1, 1))
                rhs0[a, coarse_rows, :] = s0
                rhs1[a, coarse_rows, :] = jnp.where(coarse_even, pltpu.roll(both, cz - 1, 1), both)
                corr0[a, coarse_rows, :] = s0 * weight
        for t in range(1, 2 * COARSE):
            right, other, out = (rhs1, corr0, corr1) if t % 2 else (rhs0, corr1, corr0)
            for region, low, high in regions((COARSE_REACH - t + 1) // 2):
                weight = inside[region]
                for first in range(low, high, 4):
                    planes = range(first, min(first + 4, high))
                    sums = neighbours(other, planes, CROW0 - 8, cwindow, t % 2, coarse_mask, 2)
                    for a, nbr in zip(planes, sums):
                        out[a, coarse_rows, :] = (right[a, coarse_rows, :] + nbr) * weight

    with phase("w_fine2"):
        arrive(second_fine, 2)

    with phase("prolong"):
        half_rows = hy + 8
        rows = pl.ds(CROW0 - 4, half_rows)
        pick = checker(half_rows, cz, 2)
        low_rows, high_rows = pl.ds(ROW0 - 8, 8), pl.ds(ROW0 + cy, 8)
        sub = lax.broadcasted_iota(jnp.int32, (8, cz), 0)
        for p in range(px + 2 * HALO):
            a, k = CPLANE0 + (p - HALO) // 2, (p - HALO) % 2
            c0, c1 = corr0[a, rows, :], corr1[a, rows, :]
            plane = jnp.where(pick, c1, c0) if k else jnp.where(pick, c0, c1)
            wide[p, pl.ds(0, half_rows, stride=2), :] = plane
            wide[p, pl.ds(1, half_rows, stride=2), :] = plane
        for p in range(px + 2 * HALO):
            low, own, high = wide[p, pl.ds(0, 8), :], wide[p, pl.ds(8, cy), :], wide[p, pl.ds(8 + cy, 8), :]
            if HALO <= p < HALO + px:
                post[p, own_rows, :] = mid[p, own_rows, :] + own
                post[p, low_rows, :] = jnp.where(sub == 7, mid[p, low_rows, :], landed[p, low_rows, :]) + low
                post[p, high_rows, :] = jnp.where(sub == 0, mid[p, high_rows, :], landed[p, high_rows, :]) + high
            else:
                post[p, own_rows, :] = landed[p, own_rows, :] + own
                post[p, low_rows, :] = landed[p, low_rows, :] + low
                post[p, high_rows, :] = landed[p, high_rows, :] + high
            if 1 <= p < px + 2 * HALO - 1:
                red[p, own_rows, :] = red[p, own_rows, :] + own
                red[p, low_rows, :] = red[p, low_rows, :] + low
                red[p, high_rows, :] = red[p, high_rows, :] + high

    with phase("post"):
        rows = pl.ds(ROW0 - REACH, window)
        for t in range(REACH - 1):
            right, other, out = (black_rhs, red, post) if t % 2 else (mix, post, red)
            for region, planes in plane_groups(t):
                keep = active[region] > 0.5
                sums = neighbours(other, planes, ROW0 - REACH, window, t % 2, fine_mask, 1)
                for p, nbr in zip(planes, sums):
                    total = right[p, rows, :] - mean + nbr
                    out[p, rows, :] = jnp.where(keep, total * SIXTH, out[p, rows, :])
        black_sweep(black_rhs, red, post)

    with phase("w_sent"):
        sent(marks_round, first_round, second_coarse, second_fine)
        if via:
            for side in (-1, 1):
                @pl.when(passes(side))
                def _():
                    passed().wait_send()
        all_sums.wait_send()


def put(red, post, defect, contrast, smoothed_out, residual_out, smoothed, residual, sem):
    px, cy, cz = contrast.shape
    own_rows = pl.ds(ROW0, cy)
    mask = checker(cy, cz)
    copies = []

    def send(n, src, dst, first, size):
        part = pl.ds(2 * first, 2 * size)
        copies.append(pltpu.make_async_copy(src.at[part], dst.at[part], sem.at[n]))
        copies[-1].start()

    for a in range(px):
        centre, value = red[HALO + a, own_rows, :], post[HALO + a, own_rows, :]
        smoothed[2 * a] = jnp.where(mask, centre, value)
        smoothed[2 * a + 1] = jnp.where(mask, value, centre)
    send(0, smoothed, smoothed_out, 0, px)
    size = px // PIECES
    for piece in range(PIECES):
        planes = range(piece * size, (piece + 1) * size)
        sums = neighbours(post, [HALO + a for a in planes], ROW0, cy, 0, mask, 1)
        for a, nbr in zip(planes, sums):
            res, other = contrast[a] + nbr - 6.0 * red[HALO + a, own_rows, :], defect[a, pl.ds(REACH, cy), :]
            residual[2 * a] = jnp.where(mask, res, other)
            residual[2 * a + 1] = jnp.where(mask, other, res)
        send(1 + piece, residual, residual_out, piece * size, size)
    for c in copies:
        c.wait()


def per_device(dims, source, potential, refined):
    cx, cy, cz = source.shape
    groups, members = dims
    px, hx, hy = cx // 2, cx // 4, cy // 2
    fine = (px + 2 * HALO, ROW0 + cy + ROW0, cz)
    coarse = (hx + 2 * CPLANE0, hy + 2 * CROW0, cz)
    f32 = jnp.float32
    dma = pltpu.SemaphoreType.DMA
    any_spec = pl.BlockSpec(memory_space=pl.ANY)
    vmem_spec = pl.BlockSpec(memory_space=pltpu.VMEM)
    results = pl.pallas_call(
        functools.partial(kernel, dims, (cx, cy, cz)),
        out_shape=[
            pltpu.VMEM(fine, f32),
            pltpu.VMEM(fine, f32),
            pltpu.VMEM((px, cy + 2 * REACH, cz), f32),
            pltpu.VMEM((px, cy, cz), f32),
        ],
        in_specs=[any_spec] * 3,
        out_specs=[vmem_spec] * 4,
        scratch_shapes=[
            pltpu.SMEM(refined.shape, jnp.int32),
            pltpu.VMEM((2, cx, cy, cz), f32),
            pltpu.VMEM((3, *fine), f32),
            pltpu.VMEM(fine, f32),
            pltpu.VMEM(fine, f32),
            pltpu.VMEM((px, cy, cz), f32),
            pltpu.VMEM(coarse, f32),
            pltpu.VMEM(coarse, f32),
            pltpu.VMEM(coarse, f32),
            pltpu.VMEM(coarse, f32),
            pltpu.VMEM(coarse, f32),
            pltpu.VMEM((px + 2 * HALO, cy + 16, cz), f32),
            pltpu.VMEM((3, 3, 8, cz), f32),
            pltpu.VMEM((3, cy + 2 * REACH, cz), f32),
            pltpu.VMEM((3, hy + 16, cz), f32),
            pltpu.VMEM((members, 8, cz), f32),
            pltpu.VMEM((groups, 8, cz), f32),
            pltpu.VMEM((groups, members, cz), f32),
            pltpu.VMEM((px, 16, cz), f32),
            pltpu.VMEM(fine, f32),
            pltpu.VMEM(fine, f32),
            pltpu.VMEM((2, px, cy, cz), f32),
            pltpu.VMEM((64 * cy, cz), f32),
            dma((3,)),
            dma((len(SIDES),)),
            dma((5,)),
            dma((4,)),
            dma((2,)),
            pltpu.SemaphoreType.REGULAR,
        ],
        compiler_params=pltpu.CompilerParams(collective_id=0, has_side_effects=True),
    )(refined, source, potential)
    return tuple(pl.pallas_call(
        put,
        out_shape=[jax.ShapeDtypeStruct(source.shape, f32)] * 2,
        in_specs=[vmem_spec] * 4,
        out_specs=[any_spec] * 2,
        scratch_shapes=[pltpu.VMEM(source.shape, f32), pltpu.VMEM(source.shape, f32), dma((1 + PIECES,))],
    )(*(pltpu.with_memory_space_constraint(v, pltpu.VMEM) for v in results)))


def solution(mesh):
    spec = P("group", "member", None)
    return jax.shard_map(
        functools.partial(per_device, (mesh.shape["group"], mesh.shape["member"])),
        mesh=mesh,
        in_specs=(spec, spec, spec),
        out_specs=(spec, spec),
        check_vma=False,
    )
```
